32 devices in a mesh: seg: 8 (over z, y), doc: 4 (over x, core).
Axes of the slice: x: 2, y: 2, z: 4, core: 2. Of those that a mesh axis runs over, the one named last changes fastest.
Arguments:
- tokens: bfloat16 [4, 2048, 768], P('doc', 'seg'), may hold values from -6 to 6
- cotangent: bfloat16 [4, 2048, 768], P('doc', 'seg'), may hold values from -6 to 6
- segment_document: int32 [4, 16], P('doc', 'seg'), may hold values from 0 to 3, never falling along the last dimension, each value on 1 to 8 neighbouring positions
- input_weight: bfloat16 [2, 768, 2304], replicated, may hold values from -0.21875 to 0.21875
- input_bias: bfloat16 [2, 2, 768], replicated, may hold values from -3 to 3
- output_weight: bfloat16 [2, 768, 768], replicated, may hold values from -1.25 to 1.25
- output_bias: bfloat16 [2, 768], replicated, may hold values from -3 to 3
- expand_weight: bfloat16 [2, 768, 3072], replicated, may hold values from -0.21875 to 0.21875
- expand_bias: bfloat16 [2, 3072], replicated, may hold values from -3 to 3
- reduce_weight: bfloat16 [2, 3072, 768], replicated, may hold values from -0.109375 to 0.109375
- reduce_bias: bfloat16 [2, 768], replicated, may hold values from -3 to 3
- norm_gain: bfloat16 [2, 2, 768], replicated, may hold values from 0.25 to 1.75
- norm_shift: bfloat16 [2, 2, 768], replicated, may hold values from -3 to 3
- position_table: bfloat16 [64, 768], replicated, may hold values from -6 to 6
Outputs:
- mixed: bfloat16 [4, 2048, 768], P('doc', 'seg')
- grad_tokens: float32 [4, 2048, 768], P('doc', 'seg')
- grad_input_weight: float32 [2, 768, 2304], P(None, 'seg', 'doc')
- grad_input_bias: float32 [2, 2, 768], P(None, None, 'seg')
- grad_output_weight: float32 [2, 768, 768], P(None, 'seg', 'doc')
- grad_output_bias: float32 [2, 768], P(None, 'seg')
- grad_expand_weight: float32 [2, 768, 3072], P(None, 'seg', 'doc')
- grad_expand_bias: float32 [2, 3072], P(None, 'seg')
- grad_reduce_weight: float32 [2, 3072, 768], P(None, 'seg', 'doc')
- grad_reduce_bias: float32 [2, 768], P(None, 'seg')
- grad_norm_gain: float32 [2, 2, 768], P(None, None, 'seg')
- grad_norm_shift: float32 [2, 2, 768], P(None, None, 'seg')
- grad_position_table: float32 [64, 768], P('doc', 'seg')
The draws below stay inside these ranges and needn't reach their ends.
Inputs may be any that keep to these rules, and one draw needn't show every extreme that they name: `segment_document`: in each group the document numbers never fall along the segments, each document has 1 to 8 segments and some document has exactly 8.
All inputs are finite; a program needn't handle non-finite values.
Results may differ from the reference program's by a relative error of at most 0.025.
Values may be sent and summed in bfloat16 or wider, within the bound.
A program may use at most 256 MiB of HBM per device.

```python
import math
import jax
import jax.numpy as jnp
import numpy as np
from jax import lax

D = 768
HEADS = 12
FF = 3072
SEG_LEN = 128
MAXPOS = 64
SEGS = 16
ROWS = 2048
GROUPS = 4
DOCS = 4
MOST_SEGS = 8


def with_spikes(entries, rng, source, target, shards_of, factor):
    def block_of(dim):
        return (jnp.arange(entries.shape[dim]) // (entries.shape[dim] // shards_of)).reshape((-1,) + (1,) * (entries.ndim - 1 - dim))

    near = jax.random.permutation(rng, shards_of)[block_of(target)]
    second = (block_of(target) + shards_of // 2) % shards_of
    return jnp.where((block_of(source) == near) | (block_of(source) == second), factor * entries, entries)


def levels(stream_key, extent, split, smallest, high):
    def one(dim, shards_of):
        heights = jax.random.uniform(jax.random.fold_in(jax.random.fold_in(stream_key, 6), dim), (shards_of,), jnp.float32, smallest / len(split), high / len(split))
        return jnp.repeat(jnp.exp(heights), extent[dim] // shards_of).reshape((-1,) + (1,) * (len(extent) - dim - 1))

    level = one(*split[0])
    for cut in split[1:]:
        level = level * one(*cut)
    return level


def length_profile(number_of, total, most, skew):
    loads = [(1 << 20) // math.isqrt(rank ** skew) + 1 for rank in range(2, number_of + 1)]
    spare, counts = total - most - (number_of - 1), [1] * (number_of - 1)
    while spare > 0:
        candidates = [i for i in range(number_of - 1) if counts[i] < most]
        mass, left = sum([loads[i] for i in candidates]), spare
        for i in candidates:
            more = min(most - counts[i], max(1, left * loads[i] // mass), spare)
            counts[i] = counts[i] + more
            spare = spare - more
    return np.array([most] + counts)


def uneven_parts(own_key, number_of, total, most, lean):
    if number_of == 2:
        one = jax.random.randint(own_key, (), max(1, total - most), min(most, total - 1) + 1)
        return jnp.stack([one, total - one])
    lengths = jnp.asarray(length_profile(number_of, total, most, lean), jnp.int32)
    couples = (number_of - 1) // 2
    source_of, sink = lengths[1:1 + 2 * couples:2], lengths[2:2 + 2 * couples:2]
    margin = jnp.minimum(source_of - 1, most - sink)
    shifted = jax.random.randint(jax.random.fold_in(own_key, 1), (couples,), 0, 1 << 20) % (margin + 1)
    lengths = lengths.at[1:1 + 2 * couples:2].set(source_of - shifted).at[2:2 + 2 * couples:2].set(sink + shifted)
    return lengths[jax.random.permutation(jax.random.fold_in(own_key, 2), number_of)]


def gaussian(key, dims, scale, limit, shards=(), dtype=jnp.bfloat16):
    array = jax.random.normal(key, dims, jnp.float32) * scale
    if len(shards) > 0:
        array = levels(key, dims, shards, -0.22, 0.18) * array
    return jnp.clip(array, min=-limit, max=limit).astype(dtype)


def heavy_noise(stream_key, shape, scale, limit, cuts, heavy, kind=jnp.bfloat16):
    drawn = scale * jax.random.normal(stream_key, shape, jnp.float32)
    if cuts:
        drawn = drawn * levels(stream_key, shape, cuts, -0.22, 0.18)
    return jnp.clip(with_spikes(drawn, jax.random.fold_in(stream_key, 3), *heavy), -limit, limit).astype(kind)


def setup_inputs(seed: int = 0) -> dict:
    streams_of = jax.random.split(jax.random.key(seed), 15)
    return {
        "tokens": gaussian(streams_of[0], (GROUPS, ROWS, D), 1.0, 6.0, ((0, 4), (1, 8))),
        "cotangent": heavy_noise(streams_of[1], (GROUPS, ROWS, D), 1.0, 6.0, ((0, 4), (1, 8)), (1, 2, 8, 2.0)),
        "segment_document": jax.vmap(lambda own: jnp.searchsorted(jnp.cumsum(uneven_parts(own, DOCS, SEGS, MOST_SEGS, 2)), jnp.arange(SEGS), side="right"))(jax.random.split(streams_of[2], GROUPS)).reshape((GROUPS, SEGS)).astype(jnp.int32),
        "input_weight": gaussian(streams_of[3], (2, D, 3 * D), D ** -0.5, 0.21875),
        "input_bias": gaussian(streams_of[4], (2, 2, D), 0.5, 3.0),
        "output_weight": gaussian(streams_of[5], (2, D, D), (D // 32) ** -0.5, 1.25),
        "output_bias": gaussian(streams_of[6], (2, D), 0.5, 3.0),
        "expand_weight": gaussian(streams_of[7], (2, D, FF), D ** -0.5, 0.21875),
        "expand_bias": gaussian(streams_of[8], (2, FF), 0.5, 3.0),
        "reduce_weight": gaussian(streams_of[9], (2, FF, D), FF ** -0.5, 0.109375),
        "reduce_bias": gaussian(streams_of[10], (2, D), 0.5, 3.0),
        "norm_gain": jnp.clip(1.0 + 0.15 * jax.random.normal(streams_of[11], (2, 2, D), jnp.float32), 0.25, 1.75).astype(jnp.bfloat16),
        "norm_shift": gaussian(streams_of[12], (2, 2, D), 0.5, 3.0),
        "position_table": gaussian(streams_of[13], (MAXPOS, D), 1.0, 6.0),
    }


@jax.custom_vjp
def low(v):
    return lax.optimization_barrier(v.astype(jnp.bfloat16)).astype(jnp.float32)

@jax.custom_vjp
def low_back(v):
    return v

def low_keep(v):
    return (low(v), None)

def low_pass(kept, grad):
    return (grad,)

def back_keep(v):
    return (v, None)

def back_low(kept, grad):
    return (low(grad),)
low.defvjp(low_keep, low_pass)
low_back.defvjp(back_keep, back_low)
EPS = 1e-05
NEGATIVE = -1e+30
HIGH = lax.Precision.HIGHEST

def both(value):
    return low(low_back(value))

def normalize(value, gain, shift):
    center = value - lax.optimization_barrier(jnp.mean(value, axis=-1, keepdims=True))
    spread = lax.optimization_barrier(jnp.mean(center * center, axis=-1, keepdims=True))
    return center * lax.rsqrt(spread + EPS) * gain + shift

def attend(queries, keys, values, allowed):
    scale = 1.0 / math.sqrt(queries.shape[-1])
    scores = low_back(jnp.einsum('bqhd,bkhd->bhqk', queries, keys, precision=HIGH) * scale)
    if allowed is not None:
        scores = jnp.where(allowed, scores, NEGATIVE)
    shares = jax.nn.softmax(scores, axis=-1)
    return jnp.einsum('bhqk,bkhd->bqhd', low(shares), values, precision=HIGH)

def layer(residual, project, params, index, allowed):
    width = residual.shape[-1]
    head_shape = residual.shape[:2] + (HEADS, width // HEADS)
    mix = jnp.einsum('bld,de->ble', project, params[0][index], precision=HIGH)
    queries = both(mix[..., :width] + params[1][index, 0]).reshape(head_shape)
    keys = both(mix[..., width:2 * width]).reshape(head_shape)
    values = both(mix[..., 2 * width:] + params[1][index, 1]).reshape(head_shape)
    attended = both(attend(queries, keys, values, allowed).reshape(residual.shape))
    branch = low_back(jnp.einsum('bld,de->ble', attended, params[2][index], precision=HIGH) + params[3][index])
    first = normalize(residual + branch, params[8][index, 0], params[9][index, 0])
    expanded = low_back(jnp.einsum('bld,df->blf', low(first), params[4][index], precision=HIGH) + params[5][index])
    hidden = low(jax.nn.gelu(expanded, approximate=False))
    reduced = low_back(jnp.einsum('blf,fd->bld', hidden, params[6][index], precision=HIGH) + params[7][index])
    return normalize(first + reduced, params[8][index, 1], params[9][index, 1])

def forward(rows, params, owners):
    results = []
    blocks = math.gcd(SEGS, 32)

    def segment_layer(piece):
        return layer(piece, low(piece), params, 0, None)
    for group in range(rows.shape[0]):
        pieces = rows[group].reshape(SEGS // blocks, blocks, SEG_LEN, D)
        segment_out = lax.map(jax.checkpoint(segment_layer), pieces).reshape(SEGS, SEG_LEN, D)
        leaders = low(segment_out[:, 0])
        owner = owners[group]
        order = jnp.arange(SEGS)
        same = owner[:, None] == owner[None, :]
        position = lax.optimization_barrier(jnp.sum(jnp.where(same & (order[None, :] < order[:, None]), 1, 0), axis=1)).astype(jnp.int32)
        cross_in = leaders + params[10][position]
        cross_out = layer(cross_in[None], low(cross_in)[None], params, 1, same[None, None])[0]
        joined = jnp.concatenate([cross_out[:, None], segment_out[:, 1:]], axis=1)
        results.append(joined.reshape(SEGS * SEG_LEN, D))
    return jnp.stack(results)

def reference(tokens, cotangent, segment_document, input_weight, input_bias, output_weight, output_bias, expand_weight, expand_bias, reduce_weight, reduce_bias, norm_gain, norm_shift, position_table):
    params = tuple((item.astype(jnp.float32) for item in (input_weight, input_bias, output_weight, output_bias, expand_weight, expand_bias, reduce_weight, reduce_bias, norm_gain, norm_shift, position_table)))
    rows = tokens.astype(jnp.float32)

    def run(rows_in, params_in):
        return forward(rows_in, params_in, segment_document)
    mixed, back = jax.vjp(run, rows, params)
    grad_rows, grad_params = back(cotangent.astype(jnp.float32))
    return (mixed.astype(jnp.bfloat16), grad_rows, grad_params[0], grad_params[1], grad_params[2], grad_params[3], grad_params[4], grad_params[5], grad_params[6], grad_params[7], grad_params[8], grad_params[9], grad_params[10])
```

```python
import functools
import math

import jax
import jax.numpy as jnp
from jax import lax
from jax.experimental import pallas as pl
from jax.experimental.pallas import tpu as pltpu
from jax.sharding import PartitionSpec as P

HEADS = 12
SEG_LEN = 128
EPS = 1e-05
NEGATIVE = -1e30
MESH = pl.DeviceIdType.MESH
F32 = jnp.float32
BF16 = jnp.bfloat16


def normalize(value, gain, shift):
    center = value - jnp.mean(value, axis=-1, keepdims=True)
    spread = jnp.mean(center * center, axis=-1, keepdims=True)
    return center * lax.rsqrt(spread + EPS) * gain + shift


def gelu_exact(value):
    return jax.nn.gelu(value, approximate=False)


def block_weights(index, stacked):
    return tuple(
        item[index].astype(F32) if place in (1, 3, 5, 7, 8, 9) else item[index]
        for place, item in enumerate(stacked)
    )


def dot(a, b):
    return jnp.dot(a, b, preferred_element_type=F32)


def dot_t(a, b):
    return lax.dot_general(a, b, (((1,), (1,)), ((), ())), preferred_element_type=F32)


def head_einsum(spec, a, b):
    return jnp.einsum(spec, a, b, preferred_element_type=F32)


def block_forward(residual, low, weights, allowed, batch):
    count, width = residual.shape
    size = width // HEADS
    scale = 1.0 / math.sqrt(size)
    shape = (batch, count // batch, HEADS, size)
    wi, bi, wo, bo, we, be, wr, br, gains, shifts = weights
    mix = dot(low, wi)
    queries = (mix[:, :width] + bi[0]).astype(BF16).reshape(shape)
    keys = mix[:, width : 2 * width].astype(BF16).reshape(shape)
    values = (mix[:, 2 * width :] + bi[1]).astype(BF16).reshape(shape)
    scores = head_einsum("bqhd,bkhd->bhqk", queries, keys) * scale
    if allowed is not None:
        scores = jnp.where(allowed, scores, NEGATIVE)
    top = jnp.max(scores, axis=-1, keepdims=True)
    raised = jnp.exp(scores - top)
    shares = raised / jnp.sum(raised, axis=-1, keepdims=True)
    attended = head_einsum("bhqk,bkhd->bqhd", shares.astype(BF16), values)
    attended = attended.astype(BF16).reshape(count, width)
    first_sum = residual + dot(attended, wo) + bo
    first = normalize(first_sum, gains[0], shifts[0])
    first_low = first.astype(BF16)
    expanded = dot(first_low, we) + be
    hidden = gelu_exact(expanded).astype(BF16)
    second_sum = first + dot(hidden, wr) + br
    out = normalize(second_sum, gains[1], shifts[1])
    return out, (
        low, queries, keys, values, shares, attended,
        first_sum, first_low, expanded, hidden, second_sum,
    )


def block_backward(grad_out, kept, weights):
    (
        low, queries, keys, values, shares, attended,
        first_sum, first_low, expanded, hidden, second_sum,
    ) = kept
    wi, bi, wo, bo, we, be, wr, br, gains, shifts = weights
    count, width = grad_out.shape
    scale = 1.0 / math.sqrt(queries.shape[-1])
    second_back = jax.vjp(normalize, second_sum, gains[1], shifts[1])[1]
    grad_second, gain_two, shift_two = second_back(grad_out)
    grad_reduced = grad_second.astype(BF16)
    grad_hidden = dot_t(grad_reduced, wr)
    grad_expanded = jax.vjp(gelu_exact, expanded)[1](grad_hidden)[0].astype(BF16)
    grad_first = grad_second + dot_t(grad_expanded, we)
    first_back = jax.vjp(normalize, first_sum, gains[0], shifts[0])[1]
    grad_first_sum, gain_one, shift_one = first_back(grad_first)
    grad_branch = grad_first_sum.astype(BF16)
    grad_att = dot_t(grad_branch, wo).astype(BF16).reshape(queries.shape)
    grad_shares = head_einsum("bqhd,bkhd->bhqk", grad_att, values)
    grad_values = head_einsum("bhqk,bqhd->bkhd", shares.astype(BF16), grad_att)
    inner = jnp.sum(grad_shares * shares, axis=-1, keepdims=True)
    grad_scores = (shares * (grad_shares - inner)).astype(BF16)
    grad_queries = head_einsum("bhqk,bkhd->bqhd", grad_scores, keys) * scale
    grad_keys = head_einsum("bhqk,bqhd->bkhd", grad_scores, queries) * scale
    project = jnp.concatenate(
        [part.reshape(count, width).astype(BF16) for part in (grad_queries, grad_keys, grad_values)],
        axis=1,
    )
    grad_rows = grad_first_sum + dot_t(project, wi)
    sums = [jnp.sum(item.astype(F32), axis=0) for item in (project, grad_branch, grad_expanded, grad_reduced)]
    small = (
        sums[0][:width], sums[0][2 * width :], sums[1], sums[2], sums[3],
        gain_one, gain_two, shift_one, shift_two,
    )
    return grad_rows, (low, attended, first_low, hidden), (project, grad_branch, grad_expanded, grad_reduced), small


def remote(src, dst, sems, index, device):
    return pltpu.make_async_remote_copy(
        src_ref=src, dst_ref=dst, send_sem=sems[0].at[index], recv_sem=sems[1].at[index],
        device_id=device, device_id_type=MESH,
    )


def greet(devices):
    barrier = pltpu.get_barrier_semaphore()
    for device in devices:
        pl.semaphore_signal(barrier, inc=1, device_id=device, device_id_type=MESH)
    pl.semaphore_wait(barrier, len(devices))


def gather_kernel(n_seg, x_ref, out_ref, land, send, recv):
    seg, doc = lax.axis_index("seg"), lax.axis_index("doc")
    peers = [(lax.rem(seg + k, n_seg), doc) for k in range(1, n_seg)]
    greet(peers)
    copies = [remote(x_ref, land.at[seg], (send, recv), k, peer) for k, peer in enumerate(peers)]
    for copy in copies:
        copy.start()
    for copy in copies:
        copy.wait()
    for k in range(1, n_seg):
        source = lax.rem(seg + k, n_seg)
        out_ref[source] = land[source]
    out_ref[seg] = x_ref[...]


def gather_seg(n_seg, packed):
    return pl.pallas_call(
        functools.partial(gather_kernel, n_seg),
        out_shape=jax.ShapeDtypeStruct((n_seg,) + packed.shape, packed.dtype),
        in_specs=[pl.BlockSpec(memory_space=pltpu.VMEM)],
        out_specs=pl.BlockSpec(memory_space=pltpu.VMEM),
        scratch_shapes=[
            pltpu.VMEM((n_seg,) + packed.shape, packed.dtype),
            pltpu.SemaphoreType.DMA((n_seg - 1,)),
            pltpu.SemaphoreType.DMA((n_seg - 1,)),
        ],
        compiler_params=pltpu.CompilerParams(collective_id=0, has_side_effects=True),
    )(packed)


class Reduce:
    def __init__(self, refs, sems, mine, devices):
        self.own, self.one, self.two, self.three, self.four = refs
        self.sems = sems
        self.a, self.b, self.l, self.h = mine
        self.devices = devices
        self.copies = []

    def send(self, src, dst, stage):
        copy = remote(src, dst, self.sems, len(self.copies), self.devices[stage])
        self.copies.append(copy)
        copy.start()

    def add(self, dst, sources, count):
        rows, lanes = self.four.shape
        step = next(size for size in (24576 // lanes, 16) if rows % size == 0)

        def body(i, carry):
            row = pl.ds(pl.multiple_of((i % (rows // step)) * step, step), step)
            total = None
            for source in sources:
                value = source(i // (rows // step), row).astype(F32)
                total = value if total is None else total + value
            dst(i // (rows // step), row, total)
            return carry

        lax.fori_loop(0, count * (rows // step), body, 0)

    def start_first(self):
        for b in (1 - self.b, self.b):
            self.send(self.own.at[1 - self.a, b], self.one.at[b], 0)

    def start_second(self):
        a, b = self.a, 1 - self.b
        self.copies[0].wait_recv()

        def put(i, row, total):
            self.own[a, b, i // 2, i % 2, row] = total.astype(BF16)

        self.add(put, [lambda i, row: self.own[a, b, i // 2, i % 2, row], lambda i, row: self.one[b, i // 2, i % 2, row]], 4)
        self.send(self.own.at[a, b], self.two, 1)

    def start_third(self):
        a, b, l = self.a, self.b, 1 - self.l
        self.copies[1].wait_recv()
        self.copies[2].wait_recv()

        def put(i, row, total):
            self.own[a, b, l, i, row] = total.astype(BF16)

        self.add(
            put,
            [
                lambda i, row: self.own[a, b, l, i, row],
                lambda i, row: self.one[b, l, i, row],
                lambda i, row: self.two[l, i, row],
            ],
            2,
        )
        self.send(self.own.at[a, b, l], self.three, 2)

    def start_fourth(self):
        a, b, l, h = self.a, self.b, self.l, 1 - self.h
        self.copies[3].wait_recv()

        def put(i, row, total):
            self.own[a, b, l, h, row] = total.astype(BF16)

        self.add(
            put,
            [
                lambda i, row: self.own[a, b, l, h, row],
                lambda i, row: self.one[b, l, h, row],
                lambda i, row: self.two[l, h, row],
                lambda i, row: self.three[h, row],
            ],
            1,
        )
        self.send(self.own.at[a, b, l, h], self.four, 3)

    def finish(self, put):
        a, b, l, h = self.a, self.b, self.l, self.h
        self.copies[4].wait_recv()
        self.add(
            lambda i, row, total: put(row, total),
            [
                lambda i, row: self.own[a, b, l, h, row],
                lambda i, row: self.one[b, l, h, row],
                lambda i, row: self.two[l, h, row],
                lambda i, row: self.three[h, row],
                lambda i, row: self.four[row],
            ],
            1,
        )
        for copy in self.copies:
            copy.wait_send()


def reduce_scratch(rows, lanes):
    return [
        pltpu.VMEM((2, 2, 2, 2, rows, lanes), BF16),
        pltpu.VMEM((2, 2, 2, rows, lanes), BF16),
        pltpu.VMEM((2, 2, rows, lanes), BF16),
        pltpu.VMEM((2, rows, lanes), BF16),
        pltpu.VMEM((rows, lanes), BF16),
        pltpu.SemaphoreType.DMA((5,)),
        pltpu.SemaphoreType.DMA((5,)),
    ]


def reduce_kernel(
    n_seg, n_doc,
    first_t, gexp, hidden, gred_t, io_t, gio, small, cross_low, cross_f32,
    out_e, out_r, out_io, out_low, out_f32,
    far_first_t, far_gexp, far_hidden, far_gred_t, far_io_t, far_gio,
    small_land, f32_send, low_land, f32_land,
    core_send, core_recv, small_send, small_recv, low_send, low_recv, f32_send_sem, f32_recv_sem,
    *reduce_refs,
):
    seg, doc = lax.axis_index("seg"), lax.axis_index("doc")
    core, x = doc % 2, doc // 2
    y, z = seg % 2, seg // 2
    low, high = z % 2, z // 2
    width = first_t.shape[0]
    rows = width // n_seg
    other_core = (seg, x * 2 + 1 - core)
    x_peer = (seg, (1 - x) * 2 + core)
    y_peer = (z * 2 + 1 - y, doc)
    low_peer = ((high * 2 + 1 - low) * 2 + y, doc)
    high_peer = (((1 - high) * 2 + low) * 2 + y, doc)
    seg_peers = [(lax.rem(seg + k, n_seg), doc) for k in range(1, n_seg)]
    doc_peers = [(seg, lax.rem(doc + k, n_doc)) for k in range(1, n_doc)]
    greet(seg_peers + doc_peers)

    swaps = [
        remote(src, dst, (core_send, core_recv), k, other_core)
        for k, (src, dst) in enumerate((
            (first_t, far_first_t),
            (gexp.at[1 - core], far_gexp),
            (hidden, far_hidden),
            (gred_t.at[:, 1 - core], far_gred_t),
            (io_t, far_io_t),
            (gio.at[:, 1 - core], far_gio),
        ))
    ]
    for swap in swaps:
        swap.start()
    smalls = [
        remote(small.at[peer[0]], small_land.at[seg], (small_send, small_recv), k, peer)
        for k, peer in enumerate(seg_peers)
    ]
    lows = [
        remote(cross_low.at[peer[1]], low_land.at[doc], (low_send, low_recv), k, peer)
        for k, peer in enumerate(doc_peers)
    ]
    for copy in smalls + lows:
        copy.start()

    down_x = (x, y, low, high)
    down_y = (y, x, low, high)
    x_first = (x_peer, y_peer, low_peer, high_peer)
    y_first = (y_peer, x_peer, low_peer, high_peer)
    take = lambda k, mine, devices: Reduce(
        reduce_refs[7 * k : 7 * k + 5], reduce_refs[7 * k + 5 : 7 * k + 7], mine, devices
    )
    exp = take(0, down_x, x_first)
    red = take(1, down_y, y_first)
    io_a = take(2, down_x, x_first)
    io_b = take(3, down_y, y_first)

    swaps[0].wait_recv()
    swaps[1].wait_recv()
    tile = 256
    tiles = width // tile

    def form_exp(k, carry):
        half = lax.rem(1 - x + k // tiles, 2)
        cols = pl.ds(pl.multiple_of((k % tiles) * tile, tile), tile)
        value = dot(first_t[...], gexp[core, half, :, cols]) + dot(far_first_t[...], far_gexp[half, :, cols])
        value = value.astype(BF16)
        for s in range(n_seg):
            exp.own[half, s % 2, (s // 2) % 2, s // 4, :, cols] = value[s * rows : (s + 1) * rows]
        return carry

    lax.fori_loop(0, tiles, form_exp, 0)
    exp.start_first()
    swaps[2].wait_recv()
    swaps[3].wait_recv()
    part = width // n_doc
    lanes = hidden.shape[1] // n_seg

    def form_red(k, carry):
        cols = pl.ds(pl.multiple_of(k * 2 * lanes, 2 * lanes), 2 * lanes)
        for half in range(2):
            value = dot(gred_t[half, core], hidden[:, cols]) + dot(far_gred_t[half], far_hidden[:, cols])
            value = value.astype(BF16)
            for side in range(2):
                red.own[side, half, k % 2, k // 2] = value[:, side * lanes : (side + 1) * lanes]
        return carry

    lax.fori_loop(0, n_seg // 2, form_red, 0)
    red.start_first()
    lax.fori_loop(tiles, 2 * tiles, form_exp, 0)
    swaps[4].wait_recv()
    swaps[5].wait_recv()
    cut = rows // 2

    def form_io(k, carry):
        half = lax.rem(1 - x + k // tiles, 2)
        cols = pl.ds(pl.multiple_of((k % tiles) * tile, tile), tile)
        value = dot(io_t[...], gio[half, core, :, cols]) + dot(far_io_t[...], far_gio[half, :, cols])
        value = value.astype(BF16)
        for s in range(n_seg):
            at = s * rows
            io_a.own[half, s % 2, (s // 2) % 2, s // 4, :, cols] = value[at : at + cut]
            io_b.own[s % 2, half, (s // 2) % 2, s // 4, :, cols] = value[at + cut : at + rows]
        return carry

    lax.fori_loop(0, 2 * tiles, form_io, 0)
    exp.start_second()
    red.start_second()
    io_a.start_first()
    io_b.start_first()

    for copy in smalls:
        copy.wait_recv()
    total = small[seg]
    for k in range(1, n_seg):
        total = total + small_land[lax.rem(seg + k, n_seg)]
    f32_send[0:32, :] = cross_f32[...]
    f32_send[32:48, :] = total

    exp.start_third()
    red.start_third()
    sums = [
        remote(f32_send, f32_land.at[doc], (f32_send_sem, f32_recv_sem), k, peer) for k, peer in enumerate(doc_peers)
    ]
    for copy in sums:
        copy.start()
    io_a.start_second()
    io_b.start_second()
    exp.start_fourth()
    red.start_fourth()

    def put_exp(row, total):
        out_e[row] = total

    def put_red(row, total):
        out_r[row] = total

    def put_a(row, total):
        out_io[0, row] = total

    def put_b(row, total):
        out_io[1, row] = total

    io_a.start_third()
    io_b.start_third()
    exp.finish(put_exp)
    red.finish(put_red)
    io_a.start_fourth()
    io_b.start_fourth()
    for copy in lows + sums:
        copy.wait_recv()
    for k in range(1, n_doc):
        source = lax.rem(doc + k, n_doc)
        out_low[source] = low_land[source]
        out_f32[source] = f32_land[source]
    out_low[doc] = cross_low[doc]
    out_f32[doc] = f32_send[...]
    io_a.finish(put_a)
    io_b.finish(put_b)
    for copy in swaps + smalls + lows + sums:
        copy.wait_send()


def reduce_all(n_seg, n_doc, first_t, gexp, hidden, gred_t, io_t, gio, small, cross_low, cross_f32):
    operands = (first_t, gexp, hidden, gred_t, io_t, gio, small, cross_low, cross_f32)
    width, count = first_t.shape
    rows, ff = width // n_seg, hidden.shape[1]
    vmem = pl.BlockSpec(memory_space=pltpu.VMEM)
    outs = (
        jax.ShapeDtypeStruct((rows, width), F32),
        jax.ShapeDtypeStruct((width // n_doc, ff // n_seg), F32),
        jax.ShapeDtypeStruct((2, rows // 2, width), F32),
        jax.ShapeDtypeStruct(cross_low.shape, BF16),
        jax.ShapeDtypeStruct((n_doc, 48, 128), F32),
    )
    sem = pltpu.SemaphoreType.DMA
    return pl.pallas_call(
        functools.partial(reduce_kernel, n_seg, n_doc),
        out_shape=outs,
        in_specs=[vmem] * len(operands),
        out_specs=[vmem] * len(outs),
        scratch_shapes=[
            pltpu.VMEM(first_t.shape, BF16),
            pltpu.VMEM(gexp.shape[1:], BF16),
            pltpu.VMEM(hidden.shape, BF16),
            pltpu.VMEM((2,) + gred_t.shape[2:], BF16),
            pltpu.VMEM(io_t.shape, BF16),
            pltpu.VMEM((2,) + gio.shape[2:], BF16),
            pltpu.VMEM(small.shape, F32),
            pltpu.VMEM((48, 128), F32),
            pltpu.VMEM(cross_low.shape, BF16),
            pltpu.VMEM((n_doc, 48, 128), F32),
            sem((6,)), sem((6,)),
            sem((n_seg - 1,)), sem((n_seg - 1,)),
            sem((n_doc - 1,)), sem((n_doc - 1,)),
            sem((n_doc - 1,)), sem((n_doc - 1,)),
        ]
        + reduce_scratch(rows, width)
        + reduce_scratch(width // n_doc, ff // n_seg)
        + reduce_scratch(rows // 2, width)
        + reduce_scratch(rows // 2, width),
        compiler_params=pltpu.CompilerParams(
            collective_id=1, has_side_effects=True, vmem_limit_bytes=60 << 20
        ),
    )(*operands)


def sliced(item, n_seg):
    return item.reshape(n_seg, item.shape[0] // n_seg)


def seg_slice(item, n_seg):
    size = item.shape[1] // n_seg
    return lax.dynamic_slice_in_dim(item, lax.axis_index("seg") * size, size, 1)


def doc_blocks(item, n_doc):
    count, width = item.shape
    return jnp.transpose(item.reshape(count, n_doc, width // n_doc), (1, 0, 2))


def pad_to(item, axis, size):
    pads = [(0, 0)] * item.ndim
    pads[axis] = (0, size - item.shape[axis])
    return jnp.pad(item, pads)


def per_device(n_seg, n_doc, tokens, cotangent, segment_document, *params):
    stacked, table = params[:10], params[10]
    local_weights, cross_weights = block_weights(0, stacked), block_weights(1, stacked)
    rows = tokens[0]
    count, width = rows.shape
    segments = count // SEG_LEN
    every = n_seg * segments
    fused = n_seg == 8 and n_doc == 4 and width % (n_seg * 32) == 0
    segment_out, kept = block_forward(rows.astype(F32), rows, local_weights, None, segments)
    layered = segment_out.reshape(segments, SEG_LEN, width)
    given = cotangent[0].reshape(segments, SEG_LEN, width)
    docs = jnp.broadcast_to(segment_document[0].astype(BF16)[:, None], (segments, width))
    packed = jnp.concatenate([layered[:, 0].astype(BF16), given[:, 0], docs], axis=0)
    packed = pad_to(packed, 0, -(-packed.shape[0] // 8) * 8)
    if fused:
        gathered = gather_seg(n_seg, packed)
    else:
        gathered = lax.all_gather(packed, "seg", axis=0)
    piece = lambda k: gathered[:, k * segments : (k + 1) * segments].reshape(every, width)
    leaders, cross_given = piece(0), piece(1).astype(F32)
    owners = piece(2)[:, 0].astype(jnp.int32)
    order = jnp.arange(every)
    same = owners[:, None] == owners[None, :]
    position = jnp.sum(jnp.where(same & (order[None, :] < order[:, None]), 1, 0), axis=1)
    places = jnp.arange(table.shape[0])
    cross_in = leaders.astype(F32) + dot((position[:, None] == places[None, :]).astype(BF16), table)
    cross_low_in = cross_in.astype(BF16)
    cross_out, cross_kept = block_forward(cross_in, cross_low_in, cross_weights, same[None, None], 1)
    grad_cross_in, cross_lefts, cross_rights, cross_small = block_backward(cross_given, cross_kept, cross_weights)

    start = lax.axis_index("seg") * segments
    own = lambda item: lax.dynamic_slice_in_dim(item, start, segments, 0)
    mixed = jnp.concatenate([own(cross_out)[:, None], layered[:, 1:]], axis=1)
    mixed = mixed.reshape(count, width).astype(BF16)
    grad_rows = jnp.concatenate([own(grad_cross_in)[:, None], given[:, 1:].astype(F32)], axis=1)
    grad_tokens, lefts, rights, small = block_backward(grad_rows.reshape(count, width), kept, local_weights)

    left = jnp.concatenate([seg_slice(item, n_seg) for item in cross_lefts], axis=1)
    right = jnp.concatenate([doc_blocks(item, n_doc) for item in cross_rights], axis=2)
    cross_low = jnp.concatenate([jnp.broadcast_to(left, (n_doc,) + left.shape), right], axis=2)
    cross_low = pad_to(cross_low, 2, -(-cross_low.shape[2] // 128) * 128)
    sized = [item.shape[0] // n_seg for item in small]
    half_rows = 16
    tall = lambda item: pad_to(pad_to(item, 1, -(-item.shape[1] // 128) * 128).reshape(item.shape[0], -1, 128), 1, half_rows)
    joined = lambda items: tall(jnp.concatenate([sliced(item, n_seg) for item in items], axis=1))
    small_all, cross_small_all = joined(small), joined(cross_small)
    cross_small_mine = lax.dynamic_index_in_dim(cross_small_all, lax.axis_index("seg"), 0, False)
    table_rows = jnp.concatenate([seg_slice(grad_cross_in, n_seg), position.astype(F32)[:, None]], axis=1)
    table_rows = pad_to(table_rows, 1, 128)
    cross_f32 = jnp.concatenate([table_rows, cross_small_mine], axis=0)

    project, branch, expanded, reduced = rights
    low, attended, first_low, hidden = lefts
    if fused:
        quarter = lambda item: jnp.transpose(item.reshape(count, 2, 2, -1), (1, 2, 0, 3))
        parts, branches = quarter(project), quarter(branch)
        inner, outer = parts.shape[-1], branches.shape[-1]
        gio = jnp.concatenate(
            [
                jnp.pad(parts, ((0, 0), (0, 0), (0, 0), (0, outer))),
                jnp.pad(branches, ((0, 0), (0, 0), (0, 0), (inner, 0))),
            ],
            axis=2,
        )
        out_e, out_r, out_io, every_low, every_f32 = reduce_all(
            n_seg, n_doc,
            first_low.T,
            jnp.transpose(expanded.reshape(count, 2, 2, -1), (2, 1, 0, 3)),
            hidden,
            reduced.T.reshape(2, 2, width // n_doc, count),
            jnp.concatenate([low.T, attended.T], axis=1),
            gio, small_all, cross_low, cross_f32,
        )
        out_io = out_io.reshape(width // n_seg, width)
        block0 = (out_io[:, :inner], out_io[:, inner:], out_e, out_r.T)
    else:
        def scattered(a, b):
            value = head_einsum("rd,re->de", a, b).astype(BF16)
            value = lax.psum_scatter(value, "seg", scatter_dimension=0, tiled=True)
            return lax.psum_scatter(value, "doc", scatter_dimension=1, tiled=True).astype(F32)

        block0 = tuple(scattered(a, b) for a, b in zip(lefts, rights))
        every_low = lax.all_to_all(cross_low, "doc", 0, 0)
        small_sum = lax.psum_scatter(small_all, "seg", scatter_dimension=0, tiled=True)[0]
        every_f32 = lax.all_gather(jnp.concatenate([cross_f32, small_sum], axis=0), "doc", axis=0)

    flat = every_low.reshape(n_doc * every, -1)
    block1, at_left, at_right = [], 0, left.shape[1]
    for a, b in zip(cross_lefts, cross_rights):
        wide, tight = a.shape[1] // n_seg, b.shape[1] // n_doc
        block1.append(
            head_einsum("rd,re->de", flat[:, at_left : at_left + wide], flat[:, at_right : at_right + tight])
        )
        at_left, at_right = at_left + wide, at_right + tight
    weights_out = [jnp.stack([zero, one]) for zero, one in zip(block0, block1)]

    part = width // n_seg
    rows_in = every_f32[:, :every].reshape(n_doc * every, 128)
    mine = lax.axis_index("doc") * (table.shape[0] // n_doc) + jnp.arange(table.shape[0] // n_doc)
    picks = rows_in[:, part][:, None] == mine[None, :].astype(F32)
    grad_table = jnp.einsum("rp,rd->pd", picks.astype(F32), rows_in[:, :part], precision=lax.Precision.HIGHEST)
    sums = jnp.sum(every_f32[:, every:], axis=0).reshape(2, half_rows * 128)
    vectors, at = [], 0
    for size in sized:
        vectors.append(jnp.stack([sums[1, at : at + size], sums[0, at : at + size]]))
        at += size
    return (
        mixed[None], grad_tokens[None],
        weights_out[0], jnp.stack(vectors[0:2], axis=1),
        weights_out[1], vectors[2],
        weights_out[2], vectors[3],
        weights_out[3], vectors[4],
        jnp.stack(vectors[5:7], axis=1), jnp.stack(vectors[7:9], axis=1),
        grad_table,
    )


def solution(mesh):
    placed = (P("doc", "seg", None), P("doc", "seg", None), P("doc", "seg")) + (P(),) * 11
    return jax.shard_map(
        functools.partial(per_device, mesh.shape["seg"], mesh.shape["doc"]),
        mesh=mesh,
        in_specs=placed,
        out_specs=(
            P("doc", "seg", None),
            P("doc", "seg", None),
            P(None, "seg", "doc"),
            P(None, None, "seg"),
            P(None, "seg", "doc"),
            P(None, "seg"),
            P(None, "seg", "doc"),
            P(None, "seg"),
            P(None, "seg", "doc"),
            P(None, "seg"),
            P(None, None, "seg"),
            P(None, None, "seg"),
            P("doc", "seg"),
        ),
        check_vma=False,
    )
```

```python
import functools
import math

import jax
import jax.numpy as jnp
from jax import lax
from jax.experimental import pallas as pl
from jax.experimental.pallas import tpu as pltpu
from jax.sharding import PartitionSpec as P


HEADS = 12
SEG_LEN = 128
EPS = 1e-05
NEGATIVE = -1e30
MESH = pl.DeviceIdType.MESH
F32 = jnp.float32
BF16 = jnp.bfloat16


def normalize(value, gain, shift):
    center = value - jnp.mean(value, axis=-1, keepdims=True)
    spread = jnp.mean(center * center, axis=-1, keepdims=True)
    return center * lax.rsqrt(spread + EPS) * gain + shift


def gelu_exact(value):
    return jax.nn.gelu(value, approximate=False)


def block_weights(index, stacked):
    return tuple(
        item[index].astype(F32) if place in (1, 3, 5, 7, 8, 9) else item[index]
        for place, item in enumerate(stacked)
    )


def dot(a, b):
    return jnp.dot(a, b, preferred_element_type=F32)


def dot_t(a, b):
    return lax.dot_general(a, b, (((1,), (1,)), ((), ())), preferred_element_type=F32)


def head_einsum(spec, a, b):
    return jnp.einsum(spec, a, b, preferred_element_type=F32)


def block_forward(residual, low, weights, allowed, batch):
    count, width = residual.shape
    size = width // HEADS
    scale = 1.0 / math.sqrt(size)
    shape = (batch, count // batch, HEADS, size)
    wi, bi, wo, bo, we, be, wr, br, gains, shifts = weights
    mix = dot(low, wi)
    queries = (mix[:, :width] + bi[0]).astype(BF16).reshape(shape)
    keys = mix[:, width : 2 * width].astype(BF16).reshape(shape)
    values = (mix[:, 2 * width :] + bi[1]).astype(BF16).reshape(shape)
    scores = head_einsum("bqhd,bkhd->bhqk", queries, keys) * scale
    if allowed is not None:
        scores = jnp.where(allowed, scores, NEGATIVE)
    top = jnp.max(scores, axis=-1, keepdims=True)
    raised = jnp.exp(scores - top)
    shares = raised / jnp.sum(raised, axis=-1, keepdims=True)
    attended = head_einsum("bhqk,bkhd->bqhd", shares.astype(BF16), values)
    attended = attended.astype(BF16).reshape(count, width)
    first_sum = residual + dot(attended, wo) + bo
    first = normalize(first_sum, gains[0], shifts[0])
    first_low = first.astype(BF16)
    expanded = dot(first_low, we) + be
    hidden = gelu_exact(expanded).astype(BF16)
    second_sum = first + dot(hidden, wr) + br
    out = normalize(second_sum, gains[1], shifts[1])
    return out, (
        low, queries, keys, values, shares, attended,
        first_sum, first_low, expanded, hidden, second_sum,
    )


def feed_backward(grad_out, first_sum_kept, weights):
    expanded, second_sum = first_sum_kept
    we, wr, gains, shifts = weights[4], weights[6], weights[8], weights[9]
    grad_second, gain_two, shift_two = jax.vjp(normalize, second_sum, gains[1], shifts[1])[1](grad_out)
    grad_reduced = grad_second.astype(BF16)
    grad_hidden = dot_t(grad_reduced, wr)
    grad_expanded = jax.vjp(gelu_exact, expanded)[1](grad_hidden)[0].astype(BF16)
    grad_first = grad_second + dot_t(grad_expanded, we)
    sums = [jnp.sum(item.astype(F32), axis=0) for item in (grad_expanded, grad_reduced)]
    return grad_first, grad_expanded, grad_reduced, (sums[0], sums[1], gain_two, shift_two)


def attend_backward(grad_first, kept, weights):
    _, queries, keys, values, shares, _, first_sum = kept[:7]
    wi, wo, gains, shifts = weights[0], weights[2], weights[8], weights[9]
    count, width = grad_first.shape
    scale = 1.0 / math.sqrt(queries.shape[-1])
    grad_first_sum, gain_one, shift_one = jax.vjp(normalize, first_sum, gains[0], shifts[0])[1](grad_first)
    grad_branch = grad_first_sum.astype(BF16)
    grad_att = dot_t(grad_branch, wo).astype(BF16).reshape(queries.shape)
    grad_shares = head_einsum("bqhd,bkhd->bhqk", grad_att, values)
    grad_values = head_einsum("bhqk,bqhd->bkhd", shares.astype(BF16), grad_att)
    inner = jnp.sum(grad_shares * shares, axis=-1, keepdims=True)
    grad_scores = (shares * (grad_shares - inner)).astype(BF16)
    grad_queries = head_einsum("bhqk,bkhd->bqhd", grad_scores, keys) * scale
    grad_keys = head_einsum("bhqk,bqhd->bkhd", grad_scores, queries) * scale
    project = jnp.concatenate(
        [part.reshape(count, width).astype(BF16) for part in (grad_queries, grad_keys, grad_values)],
        axis=1,
    )
    grad_rows = grad_first_sum + dot_t(project, wi)
    sums = [jnp.sum(item.astype(F32), axis=0) for item in (project, grad_branch)]
    return grad_rows, project, grad_branch, (sums[0][:width], sums[0][2 * width :], sums[1], gain_one, shift_one)


def small_order(attend, feed):
    return attend[:3] + feed[:2] + (attend[3], feed[2], attend[4], feed[3])


def remote(src, dst, sems, index, device):
    return pltpu.make_async_remote_copy(
        src_ref=src, dst_ref=dst, send_sem=sems[0].at[index], recv_sem=sems[1].at[index],
        device_id=device, device_id_type=MESH,
    )


def greet(devices):
    barrier = pltpu.get_barrier_semaphore()
    for device in devices:
        pl.semaphore_signal(barrier, inc=1, device_id=device, device_id_type=MESH)
    pl.semaphore_wait(barrier, len(devices))


def gather_kernel(n_seg, x_ref, out_ref, land, send, recv):
    seg, doc = lax.axis_index("seg"), lax.axis_index("doc")
    peers = [(lax.rem(seg + k, n_seg), doc) for k in range(1, n_seg)]
    greet(peers)
    copies = [remote(x_ref, land.at[seg], (send, recv), k, peer) for k, peer in enumerate(peers)]
    for copy in copies:
        copy.start()
    for copy in copies:
        copy.wait()
    for k in range(1, n_seg):
        source = lax.rem(seg + k, n_seg)
        out_ref[source] = land[source]
    out_ref[seg] = x_ref[...]


def gather_seg(n_seg, packed):
    return pl.pallas_call(
        functools.partial(gather_kernel, n_seg),
        out_shape=jax.ShapeDtypeStruct((n_seg,) + packed.shape, packed.dtype),
        in_specs=[pl.BlockSpec(memory_space=pltpu.VMEM)],
        out_specs=pl.BlockSpec(memory_space=pltpu.VMEM),
        scratch_shapes=[
            pltpu.VMEM((n_seg,) + packed.shape, packed.dtype),
            pltpu.SemaphoreType.DMA((n_seg - 1,)),
            pltpu.SemaphoreType.DMA((n_seg - 1,)),
        ],
        compiler_params=pltpu.CompilerParams(collective_id=0, has_side_effects=True),
    )(packed)


class Reduce:
    def __init__(self, refs, sems, mine, devices):
        self.own, self.one, self.two, self.three, self.four = refs
        self.sems = sems
        self.a, self.b, self.l, self.h = mine
        self.devices = devices
        self.copies = []

    def send(self, src, dst, stage):
        copy = remote(src, dst, self.sems, len(self.copies), self.devices[stage])
        self.copies.append(copy)
        copy.start()

    def add(self, dst, sources, count):
        rows, lanes = self.four.shape
        step = next(size for size in (24576 // lanes, 16) if rows % size == 0)

        def body(i, carry):
            row = pl.ds(pl.multiple_of((i % (rows // step)) * step, step), step)
            total = None
            for source in sources:
                value = source(i // (rows // step), row).astype(F32)
                total = value if total is None else total + value
            dst(i // (rows // step), row, total)
            return carry

        lax.fori_loop(0, count * (rows // step), body, 0)

    def start_first(self):
        for b in (1 - self.b, self.b):
            self.send(self.own.at[1 - self.a, b], self.one.at[b], 0)

    def start_second(self):
        a, b = self.a, 1 - self.b
        self.copies[0].wait_recv()

        def put(i, row, total):
            self.own[a, b, i // 2, i % 2, row] = total.astype(BF16)

        self.add(put, [lambda i, row: self.own[a, b, i // 2, i % 2, row], lambda i, row: self.one[b, i // 2, i % 2, row]], 4)
        self.send(self.own.at[a, b], self.two, 1)

    def start_third(self):
        a, b, l = self.a, self.b, 1 - self.l
        self.copies[1].wait_recv()
        self.copies[2].wait_recv()

        def put(i, row, total):
            self.own[a, b, l, i, row] = total.astype(BF16)

        self.add(
            put,
            [
                lambda i, row: self.own[a, b, l, i, row],
                lambda i, row: self.one[b, l, i, row],
                lambda i, row: self.two[l, i, row],
            ],
            2,
        )
        self.send(self.own.at[a, b, l], self.three, 2)

    def start_fourth(self):
        a, b, l, h = self.a, self.b, self.l, 1 - self.h
        self.copies[3].wait_recv()

        def put(i, row, total):
            self.own[a, b, l, h, row] = total.astype(BF16)

        self.add(
            put,
            [
                lambda i, row: self.own[a, b, l, h, row],
                lambda i, row: self.one[b, l, h, row],
                lambda i, row: self.two[l, h, row],
                lambda i, row: self.three[h, row],
            ],
            1,
        )
        self.send(self.own.at[a, b, l, h], self.four, 3)

    def finish(self, put):
        a, b, l, h = self.a, self.b, self.l, self.h
        self.copies[4].wait_recv()
        self.add(
            lambda i, row, total: put(row, total),
            [
                lambda i, row: self.own[a, b, l, h, row],
                lambda i, row: self.one[b, l, h, row],
                lambda i, row: self.two[l, h, row],
                lambda i, row: self.three[h, row],
                lambda i, row: self.four[row],
            ],
            1,
        )
        for copy in self.copies:
            copy.wait_send()


def reduce_scratch(rows, lanes):
    return [
        pltpu.VMEM((2, 2, 2, 2, rows, lanes), BF16),
        pltpu.VMEM((2, 2, 2, rows, lanes), BF16),
        pltpu.VMEM((2, 2, rows, lanes), BF16),
        pltpu.VMEM((2, rows, lanes), BF16),
        pltpu.VMEM((rows, lanes), BF16),
        pltpu.SemaphoreType.DMA((5,)),
        pltpu.SemaphoreType.DMA((5,)),
    ]


def reduce_kernel(
    n_seg, n_doc,
    io_t, gio, small, lead, cross_low, cross_f32,
    out_io, out_lead, out_low, out_f32,
    far_io_t, far_gio, small_land, lead_land, lead_two, f32_send, low_land, f32_land,
    core_send, core_recv, small_send, small_recv, lead_send, lead_recv, low_send, low_recv,
    f32_send_sem, f32_recv_sem, two_send, two_recv,
    *reduce_refs,
):
    seg, doc = lax.axis_index("seg"), lax.axis_index("doc")
    core, x = doc % 2, doc // 2
    y, z = seg % 2, seg // 2
    low, high = z % 2, z // 2
    width = io_t.shape[0]
    rows = width // n_seg
    other_core = (seg, x * 2 + 1 - core)
    x_peer = (seg, (1 - x) * 2 + core)
    y_peer = (z * 2 + 1 - y, doc)
    low_peer = ((high * 2 + 1 - low) * 2 + y, doc)
    high_peer = (((1 - high) * 2 + low) * 2 + y, doc)
    seg_peers = [(lax.rem(seg + k, n_seg), doc) for k in range(1, n_seg)]
    doc_peers = [(seg, lax.rem(doc + k, n_doc)) for k in range(1, n_doc)]
    greet(seg_peers + doc_peers)

    swaps = [
        remote(src, dst, (core_send, core_recv), k, other_core)
        for k, (src, dst) in enumerate(((io_t, far_io_t), (gio.at[:, 1 - core], far_gio)))
    ]
    smalls = [
        remote(small.at[peer[0]], small_land.at[seg], (small_send, small_recv), k, peer)
        for k, peer in enumerate(seg_peers)
    ]
    leads = [
        remote(lead.at[peer[0]], lead_land.at[seg], (lead_send, lead_recv), k, peer)
        for k, peer in enumerate(seg_peers)
    ]
    lows = [
        remote(cross_low.at[peer[1]], low_land.at[doc], (low_send, low_recv), k, peer)
        for k, peer in enumerate(doc_peers)
    ]
    for copy in swaps + smalls + leads + lows:
        copy.start()

    x_first = (x_peer, y_peer, low_peer, high_peer)
    y_first = (y_peer, x_peer, low_peer, high_peer)
    io_a = Reduce(reduce_refs[0:5], reduce_refs[5:7], (x, y, low, high), x_first)
    io_b = Reduce(reduce_refs[7:12], reduce_refs[12:14], (y, x, low, high), y_first)
    for copy in swaps:
        copy.wait_recv()
    tile = 256
    tiles = width // tile
    cut = rows // 2

    def form_io(k, carry):
        half = lax.rem(1 - x + k // tiles, 2)
        cols = pl.ds(pl.multiple_of((k % tiles) * tile, tile), tile)
        value = dot(io_t[...], gio[half, core, :, cols]) + dot(far_io_t[...], far_gio[half, :, cols])
        value = value.astype(BF16)
        for s in range(n_seg):
            at = s * rows
            io_a.own[half, s % 2, (s // 2) % 2, s // 4, :, cols] = value[at : at + cut]
            io_b.own[s % 2, half, (s // 2) % 2, s // 4, :, cols] = value[at + cut : at + rows]
        return carry

    lax.fori_loop(0, tiles, form_io, 0)
    io_a.start_first()
    lax.fori_loop(tiles, 2 * tiles, form_io, 0)
    io_b.start_first()

    for copy in smalls + leads:
        copy.wait_recv()
    total = small[seg]
    for k in range(1, n_seg):
        total = total + small_land[lax.rem(seg + k, n_seg)]
    f32_send[0:32, :] = cross_f32[...]
    f32_send[32:48, :] = total
    lead_land[seg] = lead[seg]
    sums = [
        remote(f32_send, f32_land.at[doc], (f32_send_sem, f32_recv_sem), k, peer) for k, peer in enumerate(doc_peers)
    ]
    for k, peer in enumerate(doc_peers):
        block = pl.ds(pl.multiple_of(16 + 16 * peer[1], 16), 16)
        sums.append(remote(lead_land.at[:, 0:16], lead_two.at[doc, 0], (two_send, two_recv), 2 * k, peer))
        sums.append(remote(lead_land.at[:, block], lead_two.at[doc, 1], (two_send, two_recv), 2 * k + 1, peer))
    for copy in sums:
        copy.start()
    io_a.start_second()
    io_b.start_second()
    for copy in lows:
        copy.wait_recv()
    io_a.start_third()
    io_b.start_third()
    for copy in sums:
        copy.wait_recv()
    for k in range(1, n_doc):
        source = lax.rem(doc + k, n_doc)
        out_low[source] = low_land[source]
        out_f32[source] = f32_land[source]
        out_lead[source] = lead_two[source]
    out_low[doc] = cross_low[doc]
    out_f32[doc] = f32_send[...]
    out_lead[doc, 0] = lead_land[:, 0:16]
    out_lead[doc, 1] = lead_land[:, pl.ds(pl.multiple_of(16 + 16 * doc, 16), 16)]
    io_a.start_fourth()
    io_b.start_fourth()

    def put_a(row, total):
        out_io[0, row] = total

    def put_b(row, total):
        out_io[1, row] = total

    io_a.finish(put_a)
    io_b.finish(put_b)
    for copy in swaps + smalls + leads + lows + sums:
        copy.wait_send()


def reduce_all(n_seg, n_doc, io_t, gio, small, lead, cross_low, cross_f32):
    operands = (io_t, gio, small, lead, cross_low, cross_f32)
    width = io_t.shape[0]
    rows = width // n_seg
    vmem = pl.BlockSpec(memory_space=pltpu.VMEM)
    two = (n_doc, 2, n_seg, 16, 128)
    outs = (
        jax.ShapeDtypeStruct((2, rows // 2, width), F32),
        jax.ShapeDtypeStruct(two, BF16),
        jax.ShapeDtypeStruct(cross_low.shape, BF16),
        jax.ShapeDtypeStruct((n_doc, 48, 128), F32),
    )
    sem = pltpu.SemaphoreType.DMA
    return pl.pallas_call(
        functools.partial(reduce_kernel, n_seg, n_doc),
        out_shape=outs,
        in_specs=[vmem] * len(operands),
        out_specs=[vmem] * len(outs),
        scratch_shapes=[
            pltpu.VMEM(io_t.shape, BF16),
            pltpu.VMEM((2,) + gio.shape[2:], BF16),
            pltpu.VMEM(small.shape, F32),
            pltpu.VMEM(lead.shape, BF16),
            pltpu.VMEM(two, BF16),
            pltpu.VMEM((48, 128), F32),
            pltpu.VMEM(cross_low.shape, BF16),
            pltpu.VMEM((n_doc, 48, 128), F32),
            sem((2,)), sem((2,)),
            sem((n_seg - 1,)), sem((n_seg - 1,)),
            sem((n_seg - 1,)), sem((n_seg - 1,)),
            sem((n_doc - 1,)), sem((n_doc - 1,)),
            sem((n_doc - 1,)), sem((n_doc - 1,)),
            sem((2 * (n_doc - 1),)), sem((2 * (n_doc - 1),)),
        ]
        + reduce_scratch(rows // 2, width)
        + reduce_scratch(rows // 2, width),
        compiler_params=pltpu.CompilerParams(
            collective_id=1, has_side_effects=True, vmem_limit_bytes=40 << 20
        ),
    )(*operands)


def along(axis, step, size):
    return lambda item: lax.ppermute(item, axis, [(i, i ^ step) for i in range(size)])


def columns(item, starts, size):
    return jnp.concatenate([lax.dynamic_slice_in_dim(item, at, size, 1) for at in starts], axis=1)


def plus(*items):
    total = items[0].astype(F32)
    for item in items[1:]:
        total = total + item.astype(F32)
    return total


def reduce_feed(n_seg, n_doc, first_low, hidden, expanded, reduced):
    seg, doc = lax.axis_index("seg"), lax.axis_index("doc")
    core, x, y, low, high = doc % 2, doc // 2, seg % 2, (seg // 2) % 2, seg // 4
    width, ff = first_low.shape[1], hidden.shape[1]
    rows, part, lanes = width // n_seg, width // n_doc, ff // n_seg
    swap, by_x = along("doc", 1, n_doc), along("doc", 2, n_doc)
    by_y, by_low, by_high = along("seg", 1, n_seg), along("seg", 2, n_seg), along("seg", 4, n_seg)
    both = lambda mine, theirs: jnp.concatenate([mine, swap(theirs)], axis=0)
    docs = lambda c: [k * 2 + c for k in range(2)]
    first_two = both(first_low, first_low)
    hidden_two = both(hidden, hidden)
    wide = lambda c: columns(expanded, [d * width for d in docs(c)], width)
    tight = lambda c: columns(reduced, [d * part for d in docs(c)], part)
    expanded_two = both(wide(core), wide(1 - core))
    reduced_two = both(tight(core), tight(1 - core))

    def exp_half(k):
        right = lax.dynamic_slice_in_dim(expanded_two, k * width, width, 1)
        return head_einsum("rd,re->de", first_two, right).astype(BF16)

    def red_half(k):
        right = columns(hidden_two, [(2 * i + k) * lanes for i in range(n_seg // 2)], lanes)
        return head_einsum("rd,re->de", reduced_two, right).astype(BF16)

    exp_x = by_x(exp_half(1 - x))
    red_y = by_y(red_half(1 - y))
    exp_own, red_own = exp_half(x), red_half(y)
    split = (2, 2, 2, rows, width)
    exp_own, exp_x = exp_own.reshape(split), exp_x.reshape(split)
    at_y = lambda item, k: lax.dynamic_index_in_dim(item, k, 2, False)
    exp_y = by_y(plus(at_y(exp_own, 1 - y), at_y(exp_x, 1 - y)).astype(BF16))
    kept = [at_y(exp_own, y), at_y(exp_x, y), exp_y]
    at_low = lambda item, k: lax.dynamic_index_in_dim(item, k, 1, False)
    exp_low = by_low(plus(*[at_low(item, 1 - low) for item in kept]).astype(BF16))
    kept = [at_low(item, low) for item in kept] + [exp_low]
    at_high = lambda item, k: lax.dynamic_index_in_dim(item, k, 0, False)
    exp_high = by_high(plus(*[at_high(item, 1 - high) for item in kept]).astype(BF16))
    exp_out = plus(*[at_high(item, high) for item in kept], exp_high)
    at_x = lambda item, k: lax.dynamic_slice_in_dim(item, k * part, part, 0)
    red_x = by_x(plus(at_x(red_own, 1 - x), at_x(red_y, 1 - x)).astype(BF16))
    kept = [at_x(red_own, x), at_x(red_y, x), red_x]
    at_low = lambda item, k: columns(item, [k * lanes, (2 + k) * lanes], lanes)
    red_low = by_low(plus(*[at_low(item, 1 - low) for item in kept]).astype(BF16))
    kept = [at_low(item, low) for item in kept] + [red_low]
    at_high = lambda item, k: lax.dynamic_slice_in_dim(item, k * lanes, lanes, 1)
    red_high = by_high(plus(*[at_high(item, 1 - high) for item in kept]).astype(BF16))
    red_out = plus(*[at_high(item, high) for item in kept], red_high)
    return exp_out, red_out.T


def sliced(item, n_seg):
    return item.reshape(n_seg, item.shape[0] // n_seg)


def seg_slice(item, n_seg):
    size = item.shape[1] // n_seg
    return lax.dynamic_slice_in_dim(item, lax.axis_index("seg") * size, size, 1)


def doc_blocks(item, n_doc):
    count, width = item.shape
    return jnp.transpose(item.reshape(count, n_doc, width // n_doc), (1, 0, 2))


def pad_to(item, axis, size):
    pads = [(0, 0)] * item.ndim
    pads[axis] = (0, size - item.shape[axis])
    return jnp.pad(item, pads)


def per_device(n_seg, n_doc, tokens, cotangent, segment_document, *params):
    stacked, table = params[:10], params[10]
    local_weights, cross_weights = block_weights(0, stacked), block_weights(1, stacked)
    rows = tokens[0]
    count, width = rows.shape
    segments = count // SEG_LEN
    every = n_seg * segments
    fused = n_seg == 8 and n_doc == 4 and width % (n_seg * 32) == 0
    segment_out, kept = block_forward(rows.astype(F32), rows, local_weights, None, segments)
    _, first_low, expanded, hidden, second_sum = kept[6:]
    layered = segment_out.reshape(segments, SEG_LEN, width)
    given = cotangent[0].reshape(segments, SEG_LEN, width)
    heads_zero = jnp.where(jnp.arange(count)[:, None] % SEG_LEN == 0, 0.0, cotangent[0].astype(F32))
    grad_first, grad_expanded, grad_reduced, feed_small = feed_backward(
        heads_zero, (expanded, second_sum), local_weights
    )
    if fused:
        out_e, out_r = reduce_feed(n_seg, n_doc, first_low, hidden, grad_expanded, grad_reduced)
    docs = jnp.broadcast_to(segment_document[0].astype(BF16)[:, None], (segments, width))
    packed = jnp.concatenate([layered[:, 0].astype(BF16), given[:, 0], docs], axis=0)
    packed = pad_to(packed, 0, -(-packed.shape[0] // 8) * 8)
    if fused:
        gathered = gather_seg(n_seg, packed)
    else:
        gathered = lax.all_gather(packed, "seg", axis=0)
    piece = lambda k: gathered[:, k * segments : (k + 1) * segments].reshape(every, width)
    leaders, cross_given = piece(0), piece(1).astype(F32)
    owners = piece(2)[:, 0].astype(jnp.int32)
    order = jnp.arange(every)
    same = owners[:, None] == owners[None, :]
    position = jnp.sum(jnp.where(same & (order[None, :] < order[:, None]), 1, 0), axis=1)
    places = jnp.arange(table.shape[0])
    cross_in = leaders.astype(F32) + dot((position[:, None] == places[None, :]).astype(BF16), table)
    cross_low_in = cross_in.astype(BF16)
    cross_out, cross_kept = block_forward(cross_in, cross_low_in, cross_weights, same[None, None], 1)
    cross_first, cross_expanded, cross_reduced, cross_feed = feed_backward(
        cross_given, (cross_kept[8], cross_kept[10]), cross_weights
    )
    grad_cross_in, cross_project, cross_branch, cross_attend = attend_backward(cross_first, cross_kept, cross_weights)
    cross_small = small_order(cross_attend, cross_feed)
    cross_lefts = (cross_low_in, cross_kept[5], cross_kept[7], cross_kept[9])
    cross_rights = (cross_project, cross_branch, cross_expanded, cross_reduced)

    start = lax.axis_index("seg") * segments
    own = lambda item: lax.dynamic_slice_in_dim(item, start, segments, 0)
    mixed = jnp.concatenate([own(cross_out)[:, None], layered[:, 1:]], axis=1)
    mixed = mixed.reshape(count, width).astype(BF16)
    heads = lambda item: item.reshape(segments, SEG_LEN, -1)[:, 0]
    lead_first, lead_expanded, lead_reduced, lead_small = feed_backward(
        own(grad_cross_in), (heads(expanded), heads(second_sum)), local_weights
    )
    grad_first = jnp.concatenate(
        [lead_first[:, None], grad_first.reshape(segments, SEG_LEN, width)[:, 1:]], axis=1
    ).reshape(count, width)
    grad_tokens, project, branch, attend_small = attend_backward(grad_first, kept, local_weights)
    small = small_order(attend_small, tuple(a + b for a, b in zip(feed_small, lead_small)))

    left = jnp.concatenate([seg_slice(item, n_seg) for item in cross_lefts], axis=1)
    right = jnp.concatenate([doc_blocks(item, n_doc) for item in cross_rights], axis=2)
    cross_low = jnp.concatenate([jnp.broadcast_to(left, (n_doc,) + left.shape), right], axis=2)
    cross_low = pad_to(cross_low, 2, -(-cross_low.shape[2] // 128) * 128)
    sized = [item.shape[0] // n_seg for item in small]
    half_rows = 16
    tall = lambda item: pad_to(pad_to(item, 1, -(-item.shape[1] // 128) * 128).reshape(item.shape[0], -1, 128), 1, half_rows)
    joined = lambda items: tall(jnp.concatenate([sliced(item, n_seg) for item in items], axis=1))
    small_all, cross_small_all = joined(small), joined(cross_small)
    cross_small_mine = lax.dynamic_index_in_dim(cross_small_all, lax.axis_index("seg"), 0, False)
    table_rows = jnp.concatenate([seg_slice(grad_cross_in, n_seg), position.astype(F32)[:, None]], axis=1)
    table_rows = pad_to(table_rows, 1, 128)
    cross_f32 = jnp.concatenate([table_rows, cross_small_mine], axis=0)

    attended = kept[5]
    if fused:
        quarter = lambda item: jnp.transpose(item.reshape(count, 2, 2, -1), (1, 2, 0, 3))
        parts, branches = quarter(project), quarter(branch)
        inner, outer = parts.shape[-1], branches.shape[-1]
        gio = jnp.concatenate(
            [
                jnp.pad(parts, ((0, 0), (0, 0), (0, 0), (0, outer))),
                jnp.pad(branches, ((0, 0), (0, 0), (0, 0), (inner, 0))),
            ],
            axis=2,
        )
        flat16 = lambda item: pad_to(item.reshape(item.shape[0], -1), 1, 2048)
        lead_left = jnp.concatenate(
            [doc_blocks(heads(first_low), n_seg), doc_blocks(heads(hidden), n_seg)], axis=2
        )
        lead_right = jnp.concatenate(
            [doc_blocks(lead_expanded, n_doc), doc_blocks(lead_reduced, n_doc)], axis=2
        )
        lead_wide, lead_tight = lead_left.shape[2], lead_right.shape[2]
        lead = jnp.concatenate(
            [
                flat16(lead_left).reshape(n_seg, 16, 128),
                jnp.broadcast_to(flat16(lead_right).reshape(1, n_doc * 16, 128), (n_seg, n_doc * 16, 128)),
            ],
            axis=1,
        )
        out_io, every_lead, every_low, every_f32 = reduce_all(
            n_seg, n_doc, jnp.concatenate([rows.T, attended.T], axis=1), gio, small_all, lead, cross_low, cross_f32
        )
        unflat = lambda item, size: item.reshape(n_doc * n_seg, 2048)[:, : segments * size].reshape(-1, size)
        lead_x, lead_g = unflat(every_lead[:, 0], lead_wide), unflat(every_lead[:, 1], lead_tight)
        out_io = out_io.reshape(width // n_seg, width)
        cut = width // n_seg
        block0 = (
            out_io[:, :inner],
            out_io[:, inner:],
            out_e + head_einsum("rd,re->de", lead_x[:, :cut], lead_g[:, :width]),
            out_r + head_einsum("rd,re->de", lead_x[:, cut:], lead_g[:, width:]),
        )
    else:
        def scattered(a, b):
            value = head_einsum("rd,re->de", a, b).astype(BF16)
            value = lax.psum_scatter(value, "seg", scatter_dimension=0, tiled=True)
            return lax.psum_scatter(value, "doc", scatter_dimension=1, tiled=True).astype(F32)

        replace = lambda head, item: jnp.concatenate(
            [head[:, None], item.reshape(segments, SEG_LEN, -1)[:, 1:]], axis=1
        ).reshape(count, -1)
        lefts = (rows, attended, first_low, hidden)
        rights = (project, branch, replace(lead_expanded, grad_expanded), replace(lead_reduced, grad_reduced))
        block0 = tuple(scattered(a, b) for a, b in zip(lefts, rights))
        every_low = lax.all_to_all(cross_low, "doc", 0, 0)
        small_sum = lax.psum_scatter(small_all, "seg", scatter_dimension=0, tiled=True)[0]
        every_f32 = lax.all_gather(jnp.concatenate([cross_f32, small_sum], axis=0), "doc", axis=0)

    flat = every_low.reshape(n_doc * every, -1)
    block1, at_left, at_right = [], 0, left.shape[1]
    for a, b in zip(cross_lefts, cross_rights):
        wide, tight = a.shape[1] // n_seg, b.shape[1] // n_doc
        block1.append(
            head_einsum("rd,re->de", flat[:, at_left : at_left + wide], flat[:, at_right : at_right + tight])
        )
        at_left, at_right = at_left + wide, at_right + tight
    weights_out = [jnp.stack([zero, one]) for zero, one in zip(block0, block1)]

    part = width // n_seg
    rows_in = every_f32[:, :every].reshape(n_doc * every, 128)
    mine = lax.axis_index("doc") * (table.shape[0] // n_doc) + jnp.arange(table.shape[0] // n_doc)
    picks = rows_in[:, part][:, None] == mine[None, :].astype(F32)
    grad_table = jnp.einsum("rp,rd->pd", picks.astype(F32), rows_in[:, :part], precision=lax.Precision.HIGHEST)
    sums = jnp.sum(every_f32[:, every:], axis=0).reshape(2, half_rows * 128)
    vectors, at = [], 0
    for size in sized:
        vectors.append(jnp.stack([sums[1, at : at + size], sums[0, at : at + size]]))
        at += size
    return (
        mixed[None], grad_tokens[None],
        weights_out[0], jnp.stack(vectors[0:2], axis=1),
        weights_out[1], vectors[2],
        weights_out[2], vectors[3],
        weights_out[3], vectors[4],
        jnp.stack(vectors[5:7], axis=1), jnp.stack(vectors[7:9], axis=1),
        grad_table,
    )


def solution(mesh):
    n_seg, n_doc = mesh.shape["seg"], mesh.shape["doc"]

    def body(*arrays):
        return per_device(n_seg, n_doc, *arrays)

    placed = (P("doc", "seg", None), P("doc", "seg", None), P("doc", "seg")) + (P(),) * 11
    return jax.shard_map(
        body,
        mesh=mesh,
        in_specs=placed,
        out_specs=(
            P("doc", "seg", None),
            P("doc", "seg", None),
            P(None, "seg", "doc"),
            P(None, None, "seg"),
            P(None, "seg", "doc"),
            P(None, "seg"),
            P(None, "seg", "doc"),
            P(None, "seg"),
            P(None, "seg", "doc"),
            P(None, "seg"),
            P(None, None, "seg"),
            P(None, None, "seg"),
            P("doc", "seg"),
        ),
        check_vma=False,
    )
```

```python
import functools
import math

import jax
import jax.numpy as jnp
from jax import lax
from jax.experimental import pallas as pl
from jax.experimental.pallas import tpu as pltpu
from jax.sharding import PartitionSpec as P

HEADS = 12
SEG_LEN = 128
EPS = 1e-05
NEGATIVE = -1e30
MESH = pl.DeviceIdType.MESH
F32 = jnp.float32
BF16 = jnp.bfloat16


def normalize(value, gain, shift):
    center = value - jnp.mean(value, axis=-1, keepdims=True)
    spread = jnp.mean(center * center, axis=-1, keepdims=True)
    return center * lax.rsqrt(spread + EPS) * gain + shift


def gelu_exact(value):
    return jax.nn.gelu(value, approximate=False)


def block_weights(index, stacked):
    return tuple(
        item[index].astype(F32) if place in (1, 3, 5, 7, 8, 9) else item[index]
        for place, item in enumerate(stacked)
    )


def dot(a, b):
    return jnp.dot(a, b, preferred_element_type=F32)


def dot_t(a, b):
    return lax.dot_general(a, b, (((1,), (1,)), ((), ())), preferred_element_type=F32)


def head_einsum(spec, a, b):
    return jnp.einsum(spec, a, b, preferred_element_type=F32)


def block_forward(residual, low, weights, allowed, batch):
    count, width = residual.shape
    size = width // HEADS
    scale = 1.0 / math.sqrt(size)
    shape = (batch, count // batch, HEADS, size)
    wi, bi, wo, bo, we, be, wr, br, gains, shifts = weights
    mix = dot(low, wi)
    queries = (mix[:, :width] + bi[0]).astype(BF16).reshape(shape)
    keys = mix[:, width : 2 * width].astype(BF16).reshape(shape)
    values = (mix[:, 2 * width :] + bi[1]).astype(BF16).reshape(shape)
    scores = head_einsum("bqhd,bkhd->bhqk", queries, keys) * scale
    if allowed is not None:
        scores = jnp.where(allowed, scores, NEGATIVE)
    top = jnp.max(scores, axis=-1, keepdims=True)
    raised = jnp.exp(scores - top)
    shares = raised / jnp.sum(raised, axis=-1, keepdims=True)
    attended = head_einsum("bhqk,bkhd->bqhd", shares.astype(BF16), values)
    attended = attended.astype(BF16).reshape(count, width)
    first_sum = residual + dot(attended, wo) + bo
    first = normalize(first_sum, gains[0], shifts[0])
    first_low = first.astype(BF16)
    expanded = dot(first_low, we) + be
    hidden = gelu_exact(expanded).astype(BF16)
    second_sum = first + dot(hidden, wr) + br
    out = normalize(second_sum, gains[1], shifts[1])
    return out, (
        low, queries, keys, values, shares, attended,
        first_sum, first_low, expanded, hidden, second_sum,
    )


def block_backward(grad_out, kept, weights, stop=False):
    (
        low, queries, keys, values, shares, attended,
        first_sum, first_low, expanded, hidden, second_sum,
    ) = kept
    wi, bi, wo, bo, we, be, wr, br, gains, shifts = weights
    count, width = grad_out.shape
    scale = 1.0 / math.sqrt(queries.shape[-1])
    second_back = jax.vjp(normalize, second_sum, gains[1], shifts[1])[1]
    grad_second, gain_two, shift_two = second_back(grad_out)
    grad_reduced = grad_second.astype(BF16)
    grad_hidden = dot_t(grad_reduced, wr)
    grad_expanded = jax.vjp(gelu_exact, expanded)[1](grad_hidden)[0].astype(BF16)
    grad_first = grad_second + dot_t(grad_expanded, we)
    first_back = jax.vjp(normalize, first_sum, gains[0], shifts[0])[1]
    grad_first_sum, gain_one, shift_one = first_back(grad_first)
    grad_branch = grad_first_sum.astype(BF16)
    if stop:
        sums = [jnp.sum(item.astype(F32), axis=0) for item in (grad_branch, grad_expanded, grad_reduced)]
        grad_att = dot_t(grad_branch, wo).astype(BF16)
        small = (*sums, gain_one, gain_two, shift_one, shift_two)
        return grad_first_sum, grad_att, (grad_branch, grad_expanded, grad_reduced), small
    grad_att = dot_t(grad_branch, wo).astype(BF16).reshape(queries.shape)
    grad_shares = head_einsum("bqhd,bkhd->bhqk", grad_att, values)
    grad_values = head_einsum("bhqk,bqhd->bkhd", shares.astype(BF16), grad_att)
    inner = jnp.sum(grad_shares * shares, axis=-1, keepdims=True)
    grad_scores = (shares * (grad_shares - inner)).astype(BF16)
    grad_queries = head_einsum("bhqk,bkhd->bqhd", grad_scores, keys) * scale
    grad_keys = head_einsum("bhqk,bqhd->bkhd", grad_scores, queries) * scale
    project = jnp.concatenate(
        [part.reshape(count, width).astype(BF16) for part in (grad_queries, grad_keys, grad_values)],
        axis=1,
    )
    grad_rows = grad_first_sum + dot_t(project, wi)
    sums = [jnp.sum(item.astype(F32), axis=0) for item in (project, grad_branch, grad_expanded, grad_reduced)]
    small = (
        sums[0][:width], sums[0][2 * width :], sums[1], sums[2], sums[3],
        gain_one, gain_two, shift_one, shift_two,
    )
    return grad_rows, (low, attended, first_low, hidden), (project, grad_branch, grad_expanded, grad_reduced), small


def remote(src, dst, sems, index, device):
    return pltpu.make_async_remote_copy(
        src_ref=src, dst_ref=dst, send_sem=sems[0].at[index], recv_sem=sems[1].at[index],
        device_id=device, device_id_type=MESH,
    )


def greet(devices):
    barrier = pltpu.get_barrier_semaphore()
    for device in devices:
        pl.semaphore_signal(barrier, inc=1, device_id=device, device_id_type=MESH)
    pl.semaphore_wait(barrier, len(devices))


def gather_kernel(n_seg, x_ref, out_ref, land, send, recv):
    seg, doc = lax.axis_index("seg"), lax.axis_index("doc")
    peers = [(lax.rem(seg + k, n_seg), doc) for k in range(1, n_seg)]
    greet(peers)
    copies = [remote(x_ref, land.at[seg], (send, recv), k, peer) for k, peer in enumerate(peers)]
    for copy in copies:
        copy.start()
    for copy in copies:
        copy.wait()
    for k in range(1, n_seg):
        source = lax.rem(seg + k, n_seg)
        out_ref[source] = land[source]
    out_ref[seg] = x_ref[...]


def gather_seg(n_seg, packed):
    return pl.pallas_call(
        functools.partial(gather_kernel, n_seg),
        out_shape=jax.ShapeDtypeStruct((n_seg,) + packed.shape, packed.dtype),
        in_specs=[pl.BlockSpec(memory_space=pltpu.VMEM)],
        out_specs=pl.BlockSpec(memory_space=pltpu.VMEM),
        scratch_shapes=[
            pltpu.VMEM((n_seg,) + packed.shape, packed.dtype),
            pltpu.SemaphoreType.DMA((n_seg - 1,)),
            pltpu.SemaphoreType.DMA((n_seg - 1,)),
        ],
        compiler_params=pltpu.CompilerParams(collective_id=0, has_side_effects=True),
    )(packed)


class Reduce:
    def __init__(self, refs, sems, mine, devices):
        self.own, self.one, self.two, self.three, self.four = refs
        self.sems = sems
        self.a, self.b, self.l, self.h = mine
        self.devices = devices
        self.copies = []

    def send(self, src, dst, stage):
        copy = remote(src, dst, self.sems, len(self.copies), self.devices[stage])
        self.copies.append(copy)
        copy.start()

    def add(self, dst, sources, count):
        rows, lanes = self.four.shape
        step = next(size for size in (24576 // lanes, 16) if rows % size == 0)

        def body(i, carry):
            row = pl.ds(pl.multiple_of((i % (rows // step)) * step, step), step)
            total = None
            for source in sources:
                value = source(i // (rows // step), row).astype(F32)
                total = value if total is None else total + value
            dst(i // (rows // step), row, total)
            return carry

        lax.fori_loop(0, count * (rows // step), body, 0)

    def start_first(self):
        for b in (1 - self.b, self.b):
            self.send(self.own.at[1 - self.a, b], self.one.at[b], 0)

    def start_second(self):
        a, b = self.a, 1 - self.b
        self.copies[0].wait_recv()

        def put(i, row, total):
            self.own[a, b, i // 2, i % 2, row] = total.astype(BF16)

        self.add(put, [lambda i, row: self.own[a, b, i // 2, i % 2, row], lambda i, row: self.one[b, i // 2, i % 2, row]], 4)
        self.send(self.own.at[a, b], self.two, 1)

    def start_third(self):
        a, b, l = self.a, self.b, 1 - self.l
        self.copies[1].wait_recv()
        self.copies[2].wait_recv()

        def put(i, row, total):
            self.own[a, b, l, i, row] = total.astype(BF16)

        self.add(
            put,
            [
                lambda i, row: self.own[a, b, l, i, row],
                lambda i, row: self.one[b, l, i, row],
                lambda i, row: self.two[l, i, row],
            ],
            2,
        )
        self.send(self.own.at[a, b, l], self.three, 2)

    def start_fourth(self):
        a, b, l, h = self.a, self.b, self.l, 1 - self.h
        self.copies[3].wait_recv()

        def put(i, row, total):
            self.own[a, b, l, h, row] = total.astype(BF16)

        self.add(
            put,
            [
                lambda i, row: self.own[a, b, l, h, row],
                lambda i, row: self.one[b, l, h, row],
                lambda i, row: self.two[l, h, row],
                lambda i, row: self.three[h, row],
            ],
            1,
        )
        self.send(self.own.at[a, b, l, h], self.four, 3)

    def finish(self, put):
        a, b, l, h = self.a, self.b, self.l, self.h
        self.copies[4].wait_recv()
        self.add(
            lambda i, row, total: put(row, total),
            [
                lambda i, row: self.own[a, b, l, h, row],
                lambda i, row: self.one[b, l, h, row],
                lambda i, row: self.two[l, h, row],
                lambda i, row: self.three[h, row],
                lambda i, row: self.four[row],
            ],
            1,
        )
        for copy in self.copies:
            copy.wait_send()


def reduce_scratch(rows, lanes):
    return [
        pltpu.VMEM((2, 2, 2, 2, rows, lanes), BF16),
        pltpu.VMEM((2, 2, 2, rows, lanes), BF16),
        pltpu.VMEM((2, 2, rows, lanes), BF16),
        pltpu.VMEM((2, rows, lanes), BF16),
        pltpu.VMEM((rows, lanes), BF16),
        pltpu.SemaphoreType.DMA((5,)),
        pltpu.SemaphoreType.DMA((5,)),
    ]


def reduce_kernel(
    n_seg, n_doc,
    first_t, gexp, hidden, gred_t, p_t, att_t, branch, small, cross_low, cross_f32,
    queries, keys, values, shares, grad_att, grad_sum, weight,
    out_e, out_r, out_io, out_low, out_f32, out_bias, out_tokens,
    far_first_t, far_gexp, far_hidden, far_gred_t, far_p_t, far_att_t, far_branch, far_top,
    small_land, f32_send, low_land, f32_land, project, top, bias, bias_land, bias_sum, bias_two,
    core_send, core_recv, small_send, small_recv, low_send, low_recv, f32_send_sem, f32_recv_sem,
    bias_send, bias_recv, two_send, two_recv,
    *reduce_refs,
):
    seg, doc = lax.axis_index("seg"), lax.axis_index("doc")
    core, x = doc % 2, doc // 2
    y, z = seg % 2, seg // 2
    low, high = z % 2, z // 2
    width = first_t.shape[0]
    rows = width // n_seg
    other_core = (seg, x * 2 + 1 - core)
    x_peer = (seg, (1 - x) * 2 + core)
    y_peer = (z * 2 + 1 - y, doc)
    low_peer = ((high * 2 + 1 - low) * 2 + y, doc)
    high_peer = (((1 - high) * 2 + low) * 2 + y, doc)
    seg_peers = [(lax.rem(seg + k, n_seg), doc) for k in range(1, n_seg)]
    doc_peers = [(seg, lax.rem(doc + k, n_doc)) for k in range(1, n_doc)]
    greet(seg_peers + doc_peers)

    swaps = [
        remote(src, dst, (core_send, core_recv), k, other_core)
        for k, (src, dst) in enumerate((
            (first_t, far_first_t),
            (gexp.at[1 - core], far_gexp),
            (hidden, far_hidden),
            (gred_t.at[:, 1 - core], far_gred_t),
            (p_t, far_p_t),
            (att_t, far_att_t),
            (branch.at[:, 1 - core], far_branch),
            (top.at[:, 1 - core], far_top),
        ))
    ]
    for swap in swaps[:7]:
        swap.start()
    smalls = [
        remote(small.at[peer[0]], small_land.at[seg], (small_send, small_recv), k, peer)
        for k, peer in enumerate(seg_peers)
    ]
    lows = [
        remote(cross_low.at[peer[1]], low_land.at[doc], (low_send, low_recv), k, peer)
        for k, peer in enumerate(doc_peers)
    ]
    for copy in smalls + lows:
        copy.start()

    down_x = (x, y, low, high)
    down_y = (y, x, low, high)
    x_first = (x_peer, y_peer, low_peer, high_peer)
    y_first = (y_peer, x_peer, low_peer, high_peer)
    take = lambda k, mine, devices: Reduce(
        reduce_refs[7 * k : 7 * k + 5], reduce_refs[7 * k + 5 : 7 * k + 7], mine, devices
    )
    exp = take(0, down_x, x_first)
    red = take(1, down_y, y_first)
    io_a = take(2, down_x, x_first)
    io_b = take(3, down_y, y_first)

    swaps[0].wait_recv()
    swaps[1].wait_recv()
    tile = 256
    tiles = width // tile

    def form_exp(k, carry):
        half = lax.rem(1 - x + k // tiles, 2)
        cols = pl.ds(pl.multiple_of((k % tiles) * tile, tile), tile)
        value = dot(first_t[...], gexp[core, half, :, cols]) + dot(far_first_t[...], far_gexp[half, :, cols])
        value = value.astype(BF16)
        for s in range(n_seg):
            exp.own[half, s % 2, (s // 2) % 2, s // 4, :, cols] = value[s * rows : (s + 1) * rows]
        return carry

    lax.fori_loop(0, tiles, form_exp, 0)
    exp.start_first()
    swaps[2].wait_recv()
    swaps[3].wait_recv()
    part = width // n_doc
    lanes = hidden.shape[1] // n_seg

    def form_red(k, carry):
        cols = pl.ds(pl.multiple_of(k * 2 * lanes, 2 * lanes), 2 * lanes)
        for half in range(2):
            value = dot(gred_t[half, core], hidden[:, cols]) + dot(far_gred_t[half], far_hidden[:, cols])
            value = value.astype(BF16)
            for side in range(2):
                red.own[side, half, k % 2, k // 2] = value[:, side * lanes : (side + 1) * lanes]
        return carry

    lax.fori_loop(0, n_seg // 2, form_red, 0)
    red.start_first()
    lax.fori_loop(tiles, 2 * tiles, form_exp, 0)

    count = queries.shape[0]
    size = width // HEADS
    scale = 1.0 / math.sqrt(size)
    pairs = HEADS // 2
    lane = lax.broadcasted_iota(jnp.int32, (SEG_LEN, 2 * size), 1)
    flip = lambda a, b: lax.dot_general(a, b, (((0,), (0,)), ((), ())), preferred_element_type=F32)
    bias[...] = jnp.zeros_like(bias)

    def attend(i, carry):
        row = pl.ds(pl.multiple_of((i // pairs) * SEG_LEN, SEG_LEN), SEG_LEN)
        spot = (i % pairs) * 2 * size
        cols = pl.ds(pl.multiple_of(spot, 2 * size), 2 * size)
        q, k, v, g = queries[row, cols], keys[row, cols], values[row, cols], grad_att[row, cols]
        gq = gk = gv = None
        for side in range(2):
            mine = lane < size if side == 0 else lane >= size
            only = lambda item: jnp.where(mine, item, jnp.zeros_like(item))
            share = shares[i // pairs, (i % pairs) * 2 + side]
            g_only = only(g)
            back = dot_t(g_only, v)
            inner = jnp.sum(back * share, axis=-1, keepdims=True)
            scores = (share * (back - inner)).astype(BF16)
            parts = (dot(scores, only(k)), flip(scores, only(q)), flip(share.astype(BF16), g_only))
            gq, gk, gv = parts if side == 0 else (gq + parts[0], gk + parts[1], gv + parts[2])
        gq, gk, gv = (gq * scale).astype(BF16), (gk * scale).astype(BF16), gv.astype(BF16)
        for place, item in enumerate((gq, gk, gv)):
            project[row, pl.ds(pl.multiple_of(place * width + spot, 2 * size), 2 * size)] = item
        bias[0:1, cols] += jnp.sum(gq.astype(F32), axis=0, keepdims=True)
        bias[1:2, cols] += jnp.sum(gv.astype(F32), axis=0, keepdims=True)
        return carry

    lax.fori_loop(0, (count // SEG_LEN) * pairs, attend, 0)
    own = 3 * width // n_doc
    for d in range(n_doc):
        top[d // 2, d % 2] = jnp.zeros_like(top[d // 2, d % 2])
        top[d // 2, d % 2, :, 0:own] = project[:, d * own : (d + 1) * own]
    swaps[7].start()
    biases = [remote(bias, bias_land.at[seg], (bias_send, bias_recv), k, peer) for k, peer in enumerate(seg_peers)]
    for copy in biases:
        copy.start()
    exp.start_second()
    red.start_second()
    for swap in swaps[4:]:
        swap.wait_recv()
    cut = rows // 2

    def form_io(k, carry):
        half = lax.rem(1 - x + k // tiles, 2)
        cols = pl.ds(pl.multiple_of((k % tiles) * tile, tile), tile)
        value = (
            dot(p_t[...], top[half, core, :, cols])
            + dot(far_p_t[...], far_top[half, :, cols])
            + dot(att_t[...], branch[half, core, :, cols])
            + dot(far_att_t[...], far_branch[half, :, cols])
        )
        value = value.astype(BF16)
        for s in range(n_seg):
            at = s * rows
            io_a.own[half, s % 2, (s // 2) % 2, s // 4, :, cols] = value[at : at + cut]
            io_b.own[s % 2, half, (s // 2) % 2, s // 4, :, cols] = value[at + cut : at + rows]
        return carry

    lax.fori_loop(0, tiles, form_io, 0)
    io_a.start_first()
    lax.fori_loop(tiles, 2 * tiles, form_io, 0)
    io_b.start_first()

    def form_tokens(k, carry):
        cols = pl.ds(pl.multiple_of(k * tile, tile), tile)
        out_tokens[:, cols] = grad_sum[:, cols] + dot_t(project[...], weight[cols, :])
        return carry

    lax.fori_loop(0, tiles, form_tokens, 0)

    for copy in smalls:
        copy.wait_recv()
    total = small[seg]
    for k in range(1, n_seg):
        total = total + small_land[lax.rem(seg + k, n_seg)]
    f32_send[0:32, :] = cross_f32[...]
    f32_send[32:48, :] = total

    for copy in biases:
        copy.wait_recv()
    total = bias[...]
    for k in range(1, n_seg):
        total = total + bias_land[lax.rem(seg + k, n_seg)]
    bias_sum[...] = total
    exp.start_third()
    red.start_third()
    sums = [
        remote(f32_send, f32_land.at[doc], (f32_send_sem, f32_recv_sem), k, peer) for k, peer in enumerate(doc_peers)
    ]
    sums += [
        remote(bias_sum, bias_two.at[doc], (two_send, two_recv), k, peer) for k, peer in enumerate(doc_peers)
    ]
    for copy in sums:
        copy.start()
    io_a.start_second()
    io_b.start_second()
    exp.start_fourth()
    red.start_fourth()

    def put_exp(row, total):
        out_e[row] = total

    def put_red(row, total):
        out_r[row] = total

    def put_a(row, total):
        out_io[0, row] = total

    def put_b(row, total):
        out_io[1, row] = total

    io_a.start_third()
    io_b.start_third()
    exp.finish(put_exp)
    red.finish(put_red)
    io_a.start_fourth()
    io_b.start_fourth()
    for copy in lows + sums:
        copy.wait_recv()
    for k in range(1, n_doc):
        source = lax.rem(doc + k, n_doc)
        out_low[source] = low_land[source]
        out_f32[source] = f32_land[source]
        out_bias[source] = bias_two[source]
    out_low[doc] = cross_low[doc]
    out_f32[doc] = f32_send[...]
    out_bias[doc] = bias_sum[...]
    io_a.finish(put_a)
    io_b.finish(put_b)
    for copy in swaps + smalls + biases + lows + sums:
        copy.wait_send()


def reduce_all(n_seg, n_doc, *operands):
    first_t, gexp, hidden, gred_t, p_t, att_t, branch, small, cross_low, cross_f32 = operands[:10]
    width, count = first_t.shape
    rows, ff = width // n_seg, hidden.shape[1]
    vmem = pl.BlockSpec(memory_space=pltpu.VMEM)
    outs = (
        jax.ShapeDtypeStruct((rows, width), F32),
        jax.ShapeDtypeStruct((width // n_doc, ff // n_seg), F32),
        jax.ShapeDtypeStruct((2, rows // 2, width), F32),
        jax.ShapeDtypeStruct(cross_low.shape, BF16),
        jax.ShapeDtypeStruct((n_doc, 48, 128), F32),
        jax.ShapeDtypeStruct((n_doc, 8, width), F32),
        jax.ShapeDtypeStruct((count, width), F32),
    )
    sem = pltpu.SemaphoreType.DMA
    return pl.pallas_call(
        functools.partial(reduce_kernel, n_seg, n_doc),
        out_shape=outs,
        in_specs=[vmem] * len(operands),
        out_specs=[vmem] * len(outs),
        scratch_shapes=[
            pltpu.VMEM(first_t.shape, BF16),
            pltpu.VMEM(gexp.shape[1:], BF16),
            pltpu.VMEM(hidden.shape, BF16),
            pltpu.VMEM((2,) + gred_t.shape[2:], BF16),
            pltpu.VMEM(p_t.shape, BF16),
            pltpu.VMEM(att_t.shape, BF16),
            pltpu.VMEM((2,) + branch.shape[2:], BF16),
            pltpu.VMEM((2,) + branch.shape[2:], BF16),
            pltpu.VMEM(small.shape, F32),
            pltpu.VMEM((48, 128), F32),
            pltpu.VMEM(cross_low.shape, BF16),
            pltpu.VMEM((n_doc, 48, 128), F32),
            pltpu.VMEM((count, 3 * width), BF16),
            pltpu.VMEM(branch.shape, BF16),
            pltpu.VMEM((8, width), F32),
            pltpu.VMEM((n_seg, 8, width), F32),
            pltpu.VMEM((8, width), F32),
            pltpu.VMEM((n_doc, 8, width), F32),
            sem((8,)), sem((8,)),
            sem((n_seg - 1,)), sem((n_seg - 1,)),
            sem((n_doc - 1,)), sem((n_doc - 1,)),
            sem((n_doc - 1,)), sem((n_doc - 1,)),
            sem((n_seg - 1,)), sem((n_seg - 1,)),
            sem((n_doc - 1,)), sem((n_doc - 1,)),
        ]
        + reduce_scratch(rows, width)
        + reduce_scratch(width // n_doc, ff // n_seg)
        + reduce_scratch(rows // 2, width)
        + reduce_scratch(rows // 2, width),
        compiler_params=pltpu.CompilerParams(
            collective_id=1, has_side_effects=True, vmem_limit_bytes=60 << 20
        ),
    )(*operands)


def sliced(item, n_seg):
    return item.reshape(n_seg, item.shape[0] // n_seg)


def seg_slice(item, n_seg):
    size = item.shape[1] // n_seg
    return lax.dynamic_slice_in_dim(item, lax.axis_index("seg") * size, size, 1)


def doc_blocks(item, n_doc):
    count, width = item.shape
    return jnp.transpose(item.reshape(count, n_doc, width // n_doc), (1, 0, 2))


def pad_to(item, axis, size):
    pads = [(0, 0)] * item.ndim
    pads[axis] = (0, size - item.shape[axis])
    return jnp.pad(item, pads)


def per_device(n_seg, n_doc, tokens, cotangent, segment_document, *params):
    stacked, table = params[:10], params[10]
    local_weights, cross_weights = block_weights(0, stacked), block_weights(1, stacked)
    rows = tokens[0]
    count, width = rows.shape
    segments = count // SEG_LEN
    every = n_seg * segments
    fused = n_seg == 8 and n_doc == 4 and width % (n_seg * 32) == 0
    segment_out, kept = block_forward(rows.astype(F32), rows, local_weights, None, segments)
    layered = segment_out.reshape(segments, SEG_LEN, width)
    given = cotangent[0].reshape(segments, SEG_LEN, width)
    docs = jnp.broadcast_to(segment_document[0].astype(BF16)[:, None], (segments, width))
    packed = jnp.concatenate([layered[:, 0].astype(BF16), given[:, 0], docs], axis=0)
    packed = pad_to(packed, 0, -(-packed.shape[0] // 8) * 8)
    if fused:
        gathered = gather_seg(n_seg, packed)
    else:
        gathered = lax.all_gather(packed, "seg", axis=0)
    piece = lambda k: gathered[:, k * segments : (k + 1) * segments].reshape(every, width)
    leaders, cross_given = piece(0), piece(1).astype(F32)
    owners = piece(2)[:, 0].astype(jnp.int32)
    order = jnp.arange(every)
    same = owners[:, None] == owners[None, :]
    position = jnp.sum(jnp.where(same & (order[None, :] < order[:, None]), 1, 0), axis=1)
    places = jnp.arange(table.shape[0])
    cross_in = leaders.astype(F32) + dot((position[:, None] == places[None, :]).astype(BF16), table)
    cross_low_in = cross_in.astype(BF16)
    cross_out, cross_kept = block_forward(cross_in, cross_low_in, cross_weights, same[None, None], 1)
    grad_cross_in, cross_lefts, cross_rights, cross_small = block_backward(cross_given, cross_kept, cross_weights)

    start = lax.axis_index("seg") * segments
    own = lambda item: lax.dynamic_slice_in_dim(item, start, segments, 0)
    mixed = jnp.concatenate([own(cross_out)[:, None], layered[:, 1:]], axis=1)
    mixed = mixed.reshape(count, width).astype(BF16)
    grad_rows = jnp.concatenate([own(grad_cross_in)[:, None], given[:, 1:].astype(F32)], axis=1)
    if fused:
        grad_sum, grad_att, rights, small = block_backward(grad_rows.reshape(count, width), kept, local_weights, True)
        small = (jnp.zeros((width,), F32),) * 2 + small
    else:
        grad_tokens, lefts, rights, small = block_backward(grad_rows.reshape(count, width), kept, local_weights)

    left = jnp.concatenate([seg_slice(item, n_seg) for item in cross_lefts], axis=1)
    right = jnp.concatenate([doc_blocks(item, n_doc) for item in cross_rights], axis=2)
    cross_low = jnp.concatenate([jnp.broadcast_to(left, (n_doc,) + left.shape), right], axis=2)
    cross_low = pad_to(cross_low, 2, -(-cross_low.shape[2] // 128) * 128)
    sized = [item.shape[0] // n_seg for item in small]
    half_rows = 16
    tall = lambda item: pad_to(pad_to(item, 1, -(-item.shape[1] // 128) * 128).reshape(item.shape[0], -1, 128), 1, half_rows)
    joined = lambda items: tall(jnp.concatenate([sliced(item, n_seg) for item in items], axis=1))
    small_all, cross_small_all = joined(small), joined(cross_small)
    cross_small_mine = lax.dynamic_index_in_dim(cross_small_all, lax.axis_index("seg"), 0, False)
    table_rows = jnp.concatenate([seg_slice(grad_cross_in, n_seg), position.astype(F32)[:, None]], axis=1)
    table_rows = pad_to(table_rows, 1, 128)
    cross_f32 = jnp.concatenate([table_rows, cross_small_mine], axis=0)

    if fused:
        low, queries, keys, values, shares, attended, _, first_low, _, hidden, _ = kept
        branch, expanded, reduced = rights
        branches = jnp.transpose(branch.reshape(count, 2, 2, -1), (1, 2, 0, 3))
        outer, inner = branches.shape[-1], 3 * width // n_doc
        flat_heads = lambda item: item.reshape(count, width)
        out_e, out_r, out_io, every_low, every_f32, every_bias, grad_tokens = reduce_all(
            n_seg, n_doc,
            first_low.T,
            jnp.transpose(expanded.reshape(count, 2, 2, -1), (2, 1, 0, 3)),
            hidden,
            reduced.T.reshape(2, 2, width // n_doc, count),
            low.T,
            attended.T,
            jnp.pad(branches, ((0, 0), (0, 0), (0, 0), (inner, 0))),
            small_all, cross_low, cross_f32,
            flat_heads(queries), flat_heads(keys), flat_heads(values), shares, grad_att, grad_sum, local_weights[0],
        )
        out_io = out_io.reshape(width // n_seg, width)
        block0 = (out_io[:, :inner], out_io[:, inner:], out_e, out_r.T)
    else:
        def scattered(a, b):
            value = head_einsum("rd,re->de", a, b).astype(BF16)
            value = lax.psum_scatter(value, "seg", scatter_dimension=0, tiled=True)
            return lax.psum_scatter(value, "doc", scatter_dimension=1, tiled=True).astype(F32)

        block0 = tuple(scattered(a, b) for a, b in zip(lefts, rights))
        every_low = lax.all_to_all(cross_low, "doc", 0, 0)
        small_sum = lax.psum_scatter(small_all, "seg", scatter_dimension=0, tiled=True)[0]
        every_f32 = lax.all_gather(jnp.concatenate([cross_f32, small_sum], axis=0), "doc", axis=0)

    flat = every_low.reshape(n_doc * every, -1)
    block1, at_left, at_right = [], 0, left.shape[1]
    for a, b in zip(cross_lefts, cross_rights):
        wide, tight = a.shape[1] // n_seg, b.shape[1] // n_doc
        block1.append(
            head_einsum("rd,re->de", flat[:, at_left : at_left + wide], flat[:, at_right : at_right + tight])
        )
        at_left, at_right = at_left + wide, at_right + tight
    weights_out = [jnp.stack([zero, one]) for zero, one in zip(block0, block1)]

    part = width // n_seg
    rows_in = every_f32[:, :every].reshape(n_doc * every, 128)
    mine = lax.axis_index("doc") * (table.shape[0] // n_doc) + jnp.arange(table.shape[0] // n_doc)
    picks = rows_in[:, part][:, None] == mine[None, :].astype(F32)
    grad_table = jnp.einsum("rp,rd->pd", picks.astype(F32), rows_in[:, :part], precision=lax.Precision.HIGHEST)
    sums = jnp.sum(every_f32[:, every:], axis=0).reshape(2, half_rows * 128)
    vectors, at = [], 0
    for size in sized:
        vectors.append(jnp.stack([sums[1, at : at + size], sums[0, at : at + size]]))
        at += size
    if fused:
        bias_mine = seg_slice(jnp.sum(every_bias, axis=0), n_seg)
        for k in range(2):
            vectors[k] = vectors[k].at[0].set(bias_mine[k])
    return (
        mixed[None], grad_tokens[None],
        weights_out[0], jnp.stack(vectors[0:2], axis=1),
        weights_out[1], vectors[2],
        weights_out[2], vectors[3],
        weights_out[3], vectors[4],
        jnp.stack(vectors[5:7], axis=1), jnp.stack(vectors[7:9], axis=1),
        grad_table,
    )


def solution(mesh):
    placed = (P("doc", "seg", None), P("doc", "seg", None), P("doc", "seg")) + (P(),) * 11
    return jax.shard_map(
        functools.partial(per_device, mesh.shape["seg"], mesh.shape["doc"]),
        mesh=mesh,
        in_specs=placed,
        out_specs=(
            P("doc", "seg", None),
            P("doc", "seg", None),
            P(None, "seg", "doc"),
            P(None, None, "seg"),
            P(None, "seg", "doc"),
            P(None, "seg"),
            P(None, "seg", "doc"),
            P(None, "seg"),
            P(None, "seg", "doc"),
            P(None, "seg"),
            P(None, None, "seg"),
            P(None, None, "seg"),
            P("doc", "seg"),
        ),
        check_vma=False,
    )
```
